32 devices in a mesh: seq: 8 (over z, x), chan: 2 (over y), dp: 2 (over core).
Axes of the slice: x: 2, y: 2, z: 4, core: 2. Of those that a mesh axis runs over, the one named last changes fastest.
Arguments:
- ssm_input: bfloat16 [2, 1024, 4096], P('dp', 'seq', 'chan'), may hold values from -6 to 6
- gate_z: bfloat16 [2, 1024, 4096], P('dp', 'seq', 'chan'), may hold values from -6 to 6
- b_proj: bfloat16 [2, 1024, 128], P('dp', 'seq'), may hold values from -0.52734375 to 0.52734375
- c_proj: bfloat16 [2, 1024, 128], P('dp', 'seq'), may hold values from -6 to 6
- step_size: float32 [2, 1024, 64], P('dp', 'seq', 'chan'), may hold values from 0.02 to 0.2
- log_decay: float32 [2, 1024, 64], P('dp', 'seq', 'chan'), may hold values from -1 to 0, as said below
- skip_d: float32 [64], P('chan'), may hold values from 0.5 to 1.5
- norm_gain: float32 [4096], P('chan'), may hold values from 0.5 to 1.5
- w_out: bfloat16 [4096, 2048], P('chan'), may hold values from -0.09375 to 0.09375
- d_out: bfloat16 [2, 1024, 2048], P('dp', 'seq', 'chan'), may hold values from -6 to 6
- game_lengths: int32 [2, 4], P('dp'), may hold values from 1 to 512, 1024 in all within a row
Outputs:
- out: bfloat16 [2, 1024, 2048], P('dp', 'seq', 'chan')
- grad_x: bfloat16 [2, 1024, 4096], P('dp', 'seq', 'chan')
- grad_gain: float32 [4096], P('chan')
- grad_skip: float32 [64], P('chan')
The draws below stay inside these ranges and needn't reach their ends.
Inputs may be any that keep to these rules, and one draw needn't show every extreme that they name: `game_lengths`: each row's 4 game lengths sum to 1024, and the longest is exactly 512. `log_decay`: a log decay per position and head.
All inputs are finite; a program needn't handle non-finite values.
Results may differ from the reference program's by a relative error of at most 0.017.
Values may be sent and summed in bfloat16 or wider, within the bound.
A program may use at most 64 MiB of HBM per device.

```python
import math
import jax
import jax.numpy as jnp
import numpy as np
from jax import lax

D = 2048
MIXER_HEADS = 64
HEADDIM = 64
DSTATE = 128
L_DEV = 128
GAMES = 4
BLOCK = 128
SEQUENCE_LENGTH = 1024
BATCH_SEQUENCES = 2


def draw_log_decay(key, part):
    random_keys = jax.random.split(jax.random.fold_in(key, 71), 7)
    fast_share = 0.5
    fast_pick = jax.random.uniform(random_keys[0], (BATCH_SEQUENCES, 1, MIXER_HEADS), jnp.float32) < fast_share
    fast_rate = jnp.exp(jax.random.uniform(random_keys[1], (BATCH_SEQUENCES, 1, MIXER_HEADS), jnp.float32, jnp.log(0.02), jnp.log(0.035)))
    slow_rate = jnp.exp(jax.random.uniform(random_keys[2], (BATCH_SEQUENCES, 1, MIXER_HEADS), jnp.float32, jnp.log(0.1 / SEQUENCE_LENGTH), jnp.log(0.7 / SEQUENCE_LENGTH)))
    baseline_rate = jnp.where(fast_pick, fast_rate, slow_rate)
    jaggedness = jnp.exp(jax.random.uniform(random_keys[3], (BATCH_SEQUENCES, SEQUENCE_LENGTH, MIXER_HEADS), jnp.float32, -0.7, 0.7))
    worker_level = jnp.exp(jax.random.uniform(random_keys[4], (BATCH_SEQUENCES, SEQUENCE_LENGTH // L_DEV, MIXER_HEADS), jnp.float32, -0.7, 0.7))
    worker_level = jnp.repeat(worker_level, L_DEV, axis=1)
    spike_places = jax.random.randint(random_keys[5], (BATCH_SEQUENCES, 3, MIXER_HEADS), 0, SEQUENCE_LENGTH)
    spike_depth = jax.random.uniform(random_keys[6], (BATCH_SEQUENCES, 3, MIXER_HEADS), jnp.float32, jnp.log(0.5), jnp.log(0.8))
    sequence_positions = jnp.arange(SEQUENCE_LENGTH, dtype=jnp.int32)
    spike_found = sequence_positions[None, :, None, None] == spike_places[:, None, :, :]
    spike_events = jnp.sum(jnp.where(spike_found, spike_depth[:, None, :, :], 0.0), axis=2)
    total = -baseline_rate * jaggedness * worker_level + spike_events
    return jnp.maximum(total, -1.0).astype(jnp.float32)


def shard_levels(key, dims, cuts, low, high):
    level = 1.0
    for dim, parts in cuts:
        draws = jax.random.uniform(jax.random.fold_in(jax.random.fold_in(key, 6), dim), (parts,), jnp.float32, low / len(cuts), high / len(cuts))
        level = level * jnp.repeat(jnp.exp(draws), dims[dim] // parts).reshape((-1,) + (1,) * (len(dims) - 1 - dim))
    return level


def profile(amount, total, reach, slope):
    loads = [(1 << 20) // math.isqrt(grade ** slope) + 1 for grade in range(2, amount + 1)]
    surplus, counts = total - reach - (amount - 1), [1] * (amount - 1)
    while surplus > 0:
        candidates = [i for i in range(amount - 1) if counts[i] < reach]
        pool, left = sum([loads[i] for i in candidates]), surplus
        for i in candidates:
            addition = min(reach - counts[i], max(1, left * loads[i] // pool), surplus)
            counts[i] = counts[i] + addition
            surplus = surplus - addition
    return np.array([reach] + counts)


def ragged(key, count, total, reach, lean):
    if count == 2:
        one = jax.random.randint(key, (), max(1, total - reach), min(reach, total - 1) + 1)
        return jnp.stack([one, total - one])
    tallies = jnp.asarray(profile(count, total, reach, lean), jnp.int32)
    twos = (count - 1) // 2
    source_of, receiver = tallies[1:1 + 2 * twos:2], tallies[2:2 + 2 * twos:2]
    slack = jnp.minimum(source_of - 1, reach - receiver)
    passed = jax.random.randint(jax.random.fold_in(key, 1), (twos,), 0, 1 << 20) % (slack + 1)
    tallies = tallies.at[1:1 + 2 * twos:2].set(source_of - passed).at[2:2 + 2 * twos:2].set(receiver + passed)
    return tallies[jax.random.permutation(jax.random.fold_in(key, 2), count)]


def normal_values(rng, extent, deviation, bound, cuts=(), kind=jnp.bfloat16):
    gain = shard_levels(rng, extent, cuts, -0.22, 0.18) if cuts else 1.0
    entries = jax.random.normal(rng, extent, jnp.float32) * deviation * gain
    return jnp.minimum(jnp.maximum(entries, -bound), bound).astype(kind)


def setup_inputs(seed: int = 0) -> dict:
    seeds = jax.random.split(jax.random.key(seed), 12)
    ssm_input = normal_values(seeds[0], (BATCH_SEQUENCES, SEQUENCE_LENGTH, MIXER_HEADS * HEADDIM), 1.0, 6.0, ((0, 2), (1, 8), (2, 2)))
    gate_z = normal_values(seeds[1], (BATCH_SEQUENCES, SEQUENCE_LENGTH, MIXER_HEADS * HEADDIM), 1.0, 6.0, ((0, 2), (1, 8), (2, 2)))
    b_proj = normal_values(seeds[2], (BATCH_SEQUENCES, SEQUENCE_LENGTH, DSTATE), (DSTATE ** -0.5), 0.52734375, ((0, 2), (1, 8)))
    c_proj = normal_values(seeds[3], (BATCH_SEQUENCES, SEQUENCE_LENGTH, DSTATE), 1.0, 6.0, ((0, 2), (1, 8)))
    step_size = jnp.clip(jnp.exp(math.log(0.2) - 2.3025851 * jax.random.uniform(seeds[4], (BATCH_SEQUENCES, SEQUENCE_LENGTH, MIXER_HEADS), jnp.float32) ** shard_levels(seeds[4], (BATCH_SEQUENCES, SEQUENCE_LENGTH, MIXER_HEADS), ((0, 2), (1, 8), (2, 2)), -0.2, 0.2)), 0.02, 0.2)
    log_decay = draw_log_decay(jax.random.fold_in(seeds[11], 71), 0)
    skip_d = jnp.clip(0.5 + 1.0 * jax.random.uniform(seeds[6], (MIXER_HEADS,), jnp.float32) ** shard_levels(seeds[6], (MIXER_HEADS,), ((0, 2),), -0.2, 0.2), 0.5, 1.5)
    norm_gain = jnp.clip(1.0 + 0.1 * jax.random.normal(seeds[7], (MIXER_HEADS * HEADDIM,), jnp.float32), 0.5, 1.5)
    w_out = normal_values(seeds[8], (MIXER_HEADS * HEADDIM, D), (MIXER_HEADS * HEADDIM) ** -0.5, 0.09375, ((0, 2),))
    d_out = normal_values(seeds[9], (BATCH_SEQUENCES, SEQUENCE_LENGTH, D), 1.0, 6.0, ((0, 2), (1, 8), (2, 2)))
    game_lengths = jax.vmap(lambda own: ragged(own, GAMES, SEQUENCE_LENGTH, SEQUENCE_LENGTH // 2, 2))(jax.random.split(seeds[10], BATCH_SEQUENCES)).reshape((BATCH_SEQUENCES, GAMES)).astype(jnp.int32)
    return dict(ssm_input=ssm_input, gate_z=gate_z, b_proj=b_proj, c_proj=c_proj, step_size=step_size, log_decay=log_decay, skip_d=skip_d, norm_gain=norm_gain, w_out=w_out, d_out=d_out, game_lengths=game_lengths)


NORM_EPS = 1e-05
PRECISE = lax.Precision.HIGHEST

def block_parts(c_block, b_block, dt_block, decay_block, reset_block):
    block_len = c_block.shape[0]
    running = jnp.cumsum(decay_block, axis=0)
    reset_count = jnp.cumsum(reset_block, axis=0).astype(jnp.int32)
    scores = jnp.dot(c_block, b_block.T, preferred_element_type=jnp.float32)
    indices = jnp.arange(block_len, dtype=jnp.int32)
    allowed = (indices[:, None] >= indices[None, :]) & (reset_count[:, None] == reset_count[None, :])
    log_gap = running.T[:, :, None] - running.T[:, None, :]
    mixing = jnp.where(allowed[None], jnp.exp(jnp.minimum(log_gap, 0.0)), 0.0) * scores[None] * dt_block.T[:, None, :]
    mixing = mixing.astype(jnp.bfloat16)
    end_count = reset_count[-1]
    carry_weight = jnp.where((reset_count == 0)[:, None], jnp.exp(running), 0.0)
    tail_weight = jnp.where((reset_count == end_count)[:, None], jnp.exp(running[-1][None, :] - running), 0.0)
    block_decay = jnp.where(end_count == 0, jnp.exp(running[-1]), 0.0)
    return (mixing, carry_weight, tail_weight, block_decay)

def one_sequence(ssm_input, gate_z, b_proj, c_proj, step_size, log_decay, starts, skip_d, norm_gain, w_out, d_out):
    sequence_positions = jnp.arange(SEQUENCE_LENGTH, dtype=jnp.int32)
    resets = jnp.any(sequence_positions[:, None] == starts[None, :], axis=1).astype(jnp.int32)
    count_blocks = SEQUENCE_LENGTH // BLOCK

    def blocked(array):
        return array.reshape((count_blocks, BLOCK) + array.shape[1:])
    x_heads = ssm_input.reshape(SEQUENCE_LENGTH, MIXER_HEADS, HEADDIM)
    zero_state = jnp.zeros((MIXER_HEADS, DSTATE, HEADDIM), jnp.float32)

    def forward_step(state, block_inputs):
        x_block, c_block, b_block, dt_block, decay_block, reset_block = block_inputs
        mixing, carry_weight, tail_weight, block_decay = block_parts(c_block, b_block, dt_block, decay_block, reset_block)
        inside = jnp.einsum('hts,shp->thp', mixing.astype(jnp.float32), x_block.astype(jnp.float32))
        carried = carry_weight[:, :, None] * jnp.einsum('tn,hnp->thp', c_block.astype(jnp.float32), state, precision=PRECISE)
        scaled = ((tail_weight * dt_block)[:, :, None] * x_block.astype(jnp.float32)).astype(jnp.bfloat16)
        fresh_state = jnp.einsum('sn,shp->hnp', b_block.astype(jnp.float32), scaled.astype(jnp.float32))
        return (block_decay[:, None, None] * state + fresh_state, inside + carried)
    _, ssd_blocks = lax.scan(forward_step, zero_state, (blocked(x_heads), blocked(c_proj), blocked(b_proj), blocked(step_size), blocked(log_decay), blocked(resets)))
    ssd_out = ssd_blocks.reshape(SEQUENCE_LENGTH, MIXER_HEADS, HEADDIM) + skip_d[None, :, None] * x_heads.astype(jnp.float32)
    gate_act = jax.nn.silu(gate_z.astype(jnp.float32))
    gated = ssd_out.reshape(SEQUENCE_LENGTH, MIXER_HEADS * HEADDIM) * gate_act
    inv_rms = lax.rsqrt(lax.optimization_barrier(jnp.mean(gated * gated, axis=1)) + NORM_EPS)
    normed = (gated * norm_gain).astype(jnp.bfloat16)
    projected = jnp.dot(normed, w_out, preferred_element_type=jnp.float32)
    out = (inv_rms[:, None] * projected).astype(jnp.bfloat16)
    pulled = jnp.dot(d_out, w_out.T, preferred_element_type=jnp.float32)
    out_dot = lax.optimization_barrier(jnp.sum(d_out.astype(jnp.float32) * projected, axis=1))
    d_normed = inv_rms[:, None] * pulled
    gain_part = lax.optimization_barrier(jnp.sum(gated * d_normed, axis=0))
    d_ssd = ((norm_gain * d_normed - (inv_rms ** 3 * out_dot / (MIXER_HEADS * HEADDIM))[:, None] * gated) * gate_act).astype(jnp.bfloat16)
    d_heads = d_ssd.reshape(SEQUENCE_LENGTH, MIXER_HEADS, HEADDIM)
    skip_part = lax.optimization_barrier(jnp.sum(d_heads.astype(jnp.float32) * x_heads.astype(jnp.float32), axis=(0, 2)))

    def backward_step(adjoint, block_inputs):
        d_block, c_block, b_block, dt_block, decay_block, reset_block = block_inputs
        mixing, carry_weight, tail_weight, block_decay = block_parts(c_block, b_block, dt_block, decay_block, reset_block)
        inside = jnp.einsum('hts,thp->shp', mixing.astype(jnp.float32), d_block.astype(jnp.float32))
        carried = (dt_block * tail_weight)[:, :, None] * jnp.einsum('sn,hnp->shp', b_block.astype(jnp.float32), adjoint, precision=PRECISE)
        weighted = (carry_weight[:, :, None] * d_block.astype(jnp.float32)).astype(jnp.bfloat16)
        fresh_adjoint = jnp.einsum('tn,thp->hnp', c_block.astype(jnp.float32), weighted.astype(jnp.float32))
        return (fresh_adjoint + block_decay[:, None, None] * adjoint, inside + carried)
    _, grad_blocks = lax.scan(backward_step, zero_state, (blocked(d_heads), blocked(c_proj), blocked(b_proj), blocked(step_size), blocked(log_decay), blocked(resets)), reverse=True)
    grad_heads = grad_blocks.reshape(SEQUENCE_LENGTH, MIXER_HEADS, HEADDIM) + skip_d[None, :, None] * d_heads.astype(jnp.float32)
    grad_x = grad_heads.astype(jnp.bfloat16).reshape(SEQUENCE_LENGTH, MIXER_HEADS * HEADDIM)
    return (out, grad_x, gain_part, skip_part)

def reference(ssm_input, gate_z, b_proj, c_proj, step_size, log_decay, skip_d, norm_gain, w_out, d_out, game_lengths):
    outs_list = []
    grads_list = []
    gain_total = jnp.zeros((MIXER_HEADS * HEADDIM,), jnp.float32)
    skip_total = jnp.zeros((MIXER_HEADS,), jnp.float32)
    for index in range(BATCH_SEQUENCES):
        lengths = game_lengths[index].astype(jnp.int32)
        starts = (jnp.cumsum(lengths) - lengths).astype(jnp.int32)
        out, grad_x, gain_part, skip_part = one_sequence(ssm_input[index], gate_z[index], b_proj[index], c_proj[index], step_size[index], log_decay[index], starts, skip_d, norm_gain, w_out, d_out[index])
        outs_list.append(out)
        grads_list.append(grad_x)
        gain_total = gain_total + gain_part
        skip_total = skip_total + skip_part
    return (jnp.stack(outs_list), jnp.stack(grads_list), gain_total, skip_total)
```

```python
import functools

import jax
import jax.numpy as jnp
from jax import lax
from jax.experimental import pallas as pl
from jax.experimental.pallas import tpu as pltpu
from jax.sharding import PartitionSpec as P

NORM_EPS = 1e-05
F32 = jnp.float32
BF16 = jnp.bfloat16
MESH = pl.DeviceIdType.MESH
FWD, BWD = 0, 1


def dot(a, b):
    return lax.dot_general(a, b, (((1,), (0,)), ((), ())), preferred_element_type=F32)


def dot_rows(a, b):
    return lax.dot_general(a, b, (((0,), (0,)), ((), ())), preferred_element_type=F32)


def dot_cols(a, b):
    return lax.dot_general(a, b, (((1,), (1,)), ((), ())), preferred_element_type=F32)


def split(value, terms):
    parts = []
    for _ in range(terms):
        part = value.astype(BF16)
        parts.append(part)
        value = value - part.astype(F32)
    return parts


def kernel(
    sizes,
    x_ref,
    b_ref,
    c_ref,
    dt_ref,
    ld_ref,
    skip_ref,
    gain_ref,
    gl_ref,
    z_hbm,
    w_hbm,
    do_hbm,
    out_ref,
    gx_ref,
    gg_ref,
    gs_ref,
    z_ref,
    w_ref,
    dfull,
    running_ref,
    run_row,
    decay_row,
    decay_peer,
    carry_e,
    tdt_e,
    mix_ref,
    inside_ref,
    act_ref,
    gated_ref,
    normed_ref,
    pulled_ref,
    d_ref,
    own_ref,
    tx1,
    rx1,
    txc,
    rxc,
    tx3,
    state_ref,
    stat_tx,
    stat_rx,
    proj_tx,
    proj_rx,
    red_tx,
    red_rx,
    load_sem,
    dl_sem,
    do_send,
    do_recv,
    dec_sem,
    s1_send,
    s1_recv,
    sc_send,
    sc_recv,
    s3_send,
    s3_recv,
    st_send,
    st_recv,
    pj_send,
    pj_recv,
    rd_send,
    rd_recv,
):
    n_seq, n_chan, n_dp, heads, games, chunks = sizes
    rows, width = x_ref.shape
    hd = width // heads
    half = width // 2
    cw = half // chunks
    total_width = width * n_chan
    nb = out_ref.shape[1]
    seq = lax.axis_index("seq")
    chan = lax.axis_index("chan")
    dp = lax.axis_index("dp")
    mine = lax.rem(seq, 2)
    partner = {"seq": seq + 1 - 2 * mine}
    place = seq // 2
    last = n_seq // 2 - 1

    steps = []
    hop = 1
    while hop < n_seq:
        steps.append({"seq": seq + hop - 2 * hop * lax.rem(seq // hop, 2)})
        hop *= 2
    hop = 1
    while hop < n_dp:
        steps.append({"dp": dp + hop - 2 * hop * lax.rem(dp // hop, 2)})
        hop *= 2
    chan_peers = [{"chan": lax.rem(chan + off, n_chan)} for off in range(1, n_chan)]
    greet = steps + chan_peers + [
        {"seq": lax.rem(seq + 2, n_seq)},
        {"seq": lax.rem(seq + n_seq - 2, n_seq)},
    ]
    barrier = pltpu.get_barrier_semaphore()
    for peer in greet:
        pl.semaphore_signal(barrier, inc=1, device_id=peer, device_id_type=MESH)

    loads = [
        pltpu.make_async_copy(z_hbm, z_ref, load_sem.at[0]),
        pltpu.make_async_copy(w_hbm, w_ref, load_sem.at[1]),
        pltpu.make_async_copy(do_hbm, dfull.at[0], dl_sem),
    ]
    loads[2].start()
    loads[0].start()
    loads[1].start()

    def remote(src, dst, ssem, rsem, peer):
        return pltpu.make_async_remote_copy(
            src_ref=src, dst_ref=dst, send_sem=ssem, recv_sem=rsem, device_id=peer, device_id_type=MESH
        )

    row_i = lax.broadcasted_iota(jnp.int32, (rows, rows), 0)
    col_i = lax.broadcasted_iota(jnp.int32, (rows, rows), 1)
    causal = row_i >= col_i
    tri = causal.astype(F32).astype(BF16)
    running = jnp.zeros((rows, heads), F32)
    for part in split(ld_ref[...], 3):
        running = running + dot(tri, part)
    running_ref[...] = running
    run_row[...] = running.T
    base = seq * rows
    count_col = jnp.zeros((rows, 1), jnp.int32)
    count_row = jnp.zeros((1, rows), jnp.int32)
    count_end = jnp.zeros((1, 1), jnp.int32)
    pos_col = base + lax.broadcasted_iota(jnp.int32, (rows, 1), 0)
    pos_row = base + lax.broadcasted_iota(jnp.int32, (1, rows), 1)
    pos_end = base + rows - 1 + lax.broadcasted_iota(jnp.int32, (1, 1), 0)
    begin = jnp.int32(0)
    for g in range(games):
        from_here = (begin >= base).astype(jnp.int32)
        count_col = count_col + (pos_col >= begin).astype(jnp.int32) * from_here
        count_row = count_row + (pos_row >= begin).astype(jnp.int32) * from_here
        count_end = count_end + (pos_end >= begin).astype(jnp.int32) * from_here
        begin = begin + gl_ref[0, g]
    end = running[rows - 1 : rows, :]
    carry = jnp.where(count_col == 0, jnp.exp(running), 0.0)
    tail = jnp.where(count_col == count_end, jnp.exp(end - running), 0.0)
    decay = jnp.where(count_end == 0, jnp.exp(end), 0.0)
    spread = (
        lax.broadcasted_iota(jnp.int32, (heads, width), 1) // hd
        == lax.broadcasted_iota(jnp.int32, (heads, width), 0)
    ).astype(F32).astype(BF16)

    def expand(value, terms):
        total = None
        for part in split(value, terms):
            piece = dot(part, spread)
            total = piece if total is None else total + piece
        return total

    tdt_e[...] = expand(tail * dt_ref[...], 2)
    row_pad = jnp.concatenate([decay, skip_ref[...], jnp.zeros((6, heads), F32)], axis=0)
    rows_e = expand(row_pad, 3)
    decay_row[...] = rows_e[0:1, :]
    skip_e = rows_e[1:2, :]

    def other_cols(c):
        return pl.ds(pl.multiple_of((1 - mine) * half + c * cw, cw), cw)

    def my_cols(c):
        return pl.ds(pl.multiple_of(mine * half + c * cw, cw), cw)

    def send1(d, c):
        return remote(tx1.at[d, c], rx1.at[d, c], s1_send.at[d, c], s1_recv.at[d, c], partner)

    def send3(d, c):
        return remote(
            tx3.at[d, c], state_ref.at[d, mine * chunks + c], s3_send.at[d, c], s3_recv.at[d, c], partner
        )

    def sendc(d, c):
        to = lax.rem(seq + (2 if d == FWD else n_seq - 2), n_seq)
        return remote(txc.at[d, c], rxc.at[d, c], sc_send.at[d, c], sc_recv.at[d, c], {"seq": to})

    has = (place > 0, place < last)
    dec = remote(decay_row, decay_peer, dec_sem.at[0], dec_sem.at[1], partner)

    def make(d, left, value_of):
        for c in range(chunks):
            tx1[d, c] = dot(left, value_of(other_cols(c))).astype(BF16)
            send1(d, c).start()
        for c in range(chunks):
            own_ref[c] = dot(left, value_of(my_cols(c)))

    def chain(d):
        first = mine == (0 if d == FWD else 1)
        prev, nxt = (has[0], has[1]) if d == FWD else (has[1], has[0])

        def body(c, _):
            send1(d, c).wait_recv()

            @pl.when(prev)
            def _():
                sendc(d, c).wait_recv()

            @pl.when(jnp.logical_not(prev))
            def _():
                rxc[d, c] = jnp.zeros((rxc.shape[2], cw), BF16)

            dec_me = decay_row[:, my_cols(c)]
            dec_peer = decay_peer[:, my_cols(c)]
            fresh = own_ref[c]
            fresh_peer = rx1[d, c].astype(F32)
            before = rxc[d, c].astype(F32)
            after_me = dec_me * before + fresh
            after_peer = dec_peer * before + fresh_peer

            @pl.when(nxt)
            def _():
                txc[d, c] = jnp.where(
                    first, dec_peer * after_me + fresh_peer, dec_me * after_peer + fresh
                ).astype(BF16)
                sendc(d, c).start()

            tx3[d, c] = jnp.where(first, after_me, before).astype(BF16)
            send3(d, c).start()
            state_ref[d, mine * chunks + c] = jnp.where(first, before, after_peer).astype(BF16)
            return 0

        lax.fori_loop(0, chunks, body, 0)

    pl.semaphore_wait(barrier, len(greet))
    dec.start()
    b_t = b_ref[...].T
    make(FWD, b_t, lambda cols: (tdt_e[:, cols] * x_ref[:, cols].astype(F32)).astype(BF16))
    loads[2].wait()
    do_copies = []
    for k, peer in enumerate(chan_peers):
        do_copies.append(remote(dfull.at[0], dfull.at[k + 1], do_send.at[k], do_recv.at[k], peer))
        do_copies[-1].start()

    scores = jnp.where(causal & (count_col == count_row), dot_cols(c_ref[...], b_ref[...]), 0.0)
    dt_row = dt_ref[...].T
    pos_lane = lax.broadcasted_iota(jnp.int32, (rows, 2 * hd), 1) < hd
    carry_e[...] = expand(carry, 2)
    loads[0].wait()

    def block_diag(pair):
        pair = pair.astype(F32)
        return jnp.concatenate(
            [jnp.where(pos_lane, pair, 0.0), jnp.where(pos_lane, 0.0, pair)], axis=0
        ).astype(BF16)

    for q in range(heads // 2):
        cols = slice(q * 2 * hd, (q + 1) * 2 * hd)
        mixes = []
        for h in (2 * q, 2 * q + 1):
            gap = jnp.minimum(running_ref[:, h : h + 1] - run_row[h : h + 1, :], 0.0)
            mixes.append((jnp.exp(gap) * scores * dt_row[h : h + 1, :]).astype(BF16))
            mix_ref[q, (h % 2) * rows : (h % 2 + 1) * rows, :] = mixes[-1]
        pair = x_ref[:, cols]
        inside_ref[:, cols] = dot(jnp.concatenate(mixes, axis=1), block_diag(pair)) + skip_e[
            :, cols
        ] * pair.astype(F32)
        zf = z_ref[:, cols].astype(F32)
        act_ref[:, cols] = zf / (1.0 + jnp.exp(-zf))

    dec.wait_recv()
    chain(FWD)

    loads[1].wait()
    for copy in do_copies:
        copy.wait_recv()
    tile = min(256, width)

    def pull(i, _):
        feats = pl.ds(pl.multiple_of(i * tile, tile), tile)
        total = None
        for k in range(n_chan):
            source = lax.rem(chan + n_chan - k, n_chan)
            piece = dot_cols(dfull[k], w_ref[feats, pl.ds(pl.multiple_of(source * nb, nb), nb)])
            total = piece if total is None else total + piece
        pulled_ref[:, feats] = total
        return 0

    lax.fori_loop(0, width // tile, pull, 0)

    def gate(q, sums):
        squares, dots = sums
        cols = pl.ds(pl.multiple_of(q * cw, cw), cw)
        carried = dot(c_ref[...], state_ref[FWD, q])
        gated = (inside_ref[:, cols] + carry_e[:, cols] * carried) * act_ref[:, cols]
        normed = (gated * gain_ref[:, cols]).astype(BF16)
        gated_ref[:, cols] = gated
        normed_ref[:, cols] = normed
        sq = gated * gated
        od = normed.astype(F32) * pulled_ref[:, cols]
        for k in range(cw // 128):
            squares = squares + sq[:, k * 128 : (k + 1) * 128]
            dots = dots + od[:, k * 128 : (k + 1) * 128]
        return squares, dots

    zero = jnp.zeros((rows, 128), F32)
    sums = lax.fori_loop(0, chunks, lambda c, s: gate(mine * chunks + c, s), (zero, zero))

    def gate_late(d):
        def body(c, s):
            send3(d, c).wait_recv()
            return gate((1 - mine) * chunks + c, s)

        return body

    squares, dots = lax.fori_loop(0, chunks, gate_late(FWD), sums)
    sq_col = jnp.sum(squares, axis=1, keepdims=True)
    dot_col = jnp.sum(dots, axis=1, keepdims=True)
    lane = lax.broadcasted_iota(jnp.int32, (rows, 128), 1)
    stats = jnp.where(lane == 0, sq_col, jnp.where(lane == 1, dot_col, 0.0))
    stat_tx[...] = stats.T[0:8, :]
    st_copies = []
    for k, peer in enumerate(chan_peers):
        st_copies.append(remote(stat_tx, stat_rx.at[k], st_send.at[k], st_recv.at[k], peer))
        st_copies[-1].start()
    total = stat_tx[...]
    for k, copy in enumerate(st_copies):
        copy.wait_recv()
        total = total + stat_rx[k]
    stat_cols = jnp.concatenate([total, jnp.zeros((rows - 8, rows), F32)], axis=0).T
    inv = lax.rsqrt(stat_cols[:, 0:1] / total_width + NORM_EPS)
    back = inv * inv * inv * stat_cols[:, 1:2] / total_width

    def cot(q, _):
        cols = pl.ds(pl.multiple_of(q * cw, cw), cw)
        gated = gated_ref[:, cols]
        d_normed = inv * pulled_ref[:, cols]
        d = ((gain_ref[:, cols] * d_normed - back * gated) * act_ref[:, cols]).astype(BF16)
        d_ref[:, cols] = d
        red_tx[0, 0:1, cols] = jnp.sum(gated * d_normed, axis=0, keepdims=True)
        red_tx[0, 1:2, cols] = jnp.sum(
            d.astype(F32) * x_ref[:, cols].astype(F32), axis=0, keepdims=True
        )
        return 0

    lax.fori_loop(0, 2 * chunks, cot, 0)
    c_t = c_ref[...].T
    make(BWD, c_t, lambda cols: (carry_e[:, cols] * d_ref[:, cols].astype(F32)).astype(BF16))

    def red(k):
        return remote(red_tx.at[k], red_rx.at[k], rd_send.at[k], rd_recv.at[k], steps[k])

    def reduce_step(k):
        red(k).wait_recv()
        red_tx[k + 1] = red_tx[k] + red_rx[k]
        if k + 1 < len(steps):
            red(k + 1).start()

    red(0).start()

    tile_n = min(256, nb)

    def project(block, store):
        def body(i, _):
            at = pl.ds(pl.multiple_of(block * nb + i * tile_n, tile_n), tile_n)
            store(pl.ds(pl.multiple_of(i * tile_n, tile_n), tile_n), dot(normed_ref[...], w_ref[:, at]))
            return 0

        lax.fori_loop(0, nb // tile_n, body, 0)

    pj_copies = []
    for k, peer in enumerate(chan_peers):

        def store(at, value, k=k):
            proj_tx[k, :, at] = value.astype(BF16)

        project(peer["chan"], store)
        pj_copies.append(remote(proj_tx.at[k], proj_rx.at[k], pj_send.at[k], pj_recv.at[k], peer))
        pj_copies[-1].start()

    chain(BWD)
    reduce_step(0)

    own_tiles = []
    for i in range(nb // tile_n):
        at = pl.ds(pl.multiple_of(chan * nb + i * tile_n, tile_n), tile_n)
        own_tiles.append(dot(normed_ref[...], w_ref[:, at]))
    for copy in pj_copies:
        copy.wait_recv()
    for i in range(nb // tile_n):
        at = slice(i * tile_n, (i + 1) * tile_n)
        value = own_tiles[i]
        for k in range(n_chan - 1):
            value = value + proj_rx[k, :, at].astype(F32)
        out_ref[:, at] = (inv * value).astype(BF16)
    if len(steps) > 1:
        reduce_step(1)

    for q in range(heads // 2):
        cols = slice(q * 2 * hd, (q + 1) * 2 * hd)
        pair = d_ref[:, cols]
        inside_ref[:, cols] = dot_rows(mix_ref[q], block_diag(pair)) + skip_e[:, cols] * pair.astype(F32)
    for k in range(2, len(steps)):
        reduce_step(k)

    def finish(q):
        cols = pl.ds(pl.multiple_of(q * cw, cw), cw)
        carried = dot(b_ref[...], state_ref[BWD, q])
        gx_ref[:, cols] = (inside_ref[:, cols] + tdt_e[:, cols] * carried).astype(BF16)

    def early(c, _):
        finish(mine * chunks + c)
        return 0

    def late(c, _):
        send3(BWD, c).wait_recv()
        finish((1 - mine) * chunks + c)
        return 0

    lax.fori_loop(0, chunks, early, 0)
    lax.fori_loop(0, chunks, late, 0)

    final = red_tx[len(steps)]
    gg_ref[...] = final[0:1, :]
    skip_cols = jnp.concatenate([final[1:2, :], jnp.zeros((7, width), F32)], axis=0)
    skip_sum = jnp.zeros((8, heads), F32)
    for part in split(skip_cols, 3):
        skip_sum = skip_sum + dot_cols(part, spread)
    gs_ref[...] = skip_sum[0:1, :]

    dec.wait_send()
    for copy in do_copies + st_copies + pj_copies:
        copy.wait_send()
    for k in range(len(steps)):
        red(k).wait_send()
    for d in (FWD, BWD):
        for c in range(chunks):
            send1(d, c).wait_send()
            send3(d, c).wait_send()

            @pl.when(has[1] if d == FWD else has[0])
            def _():
                sendc(d, c).wait_send()


def local(
    mesh_shape, ssm_input, gate_z, b_proj, c_proj, step_size, log_decay, skip_d, norm_gain, w_out, d_out, game_lengths
):
    n_seq, n_chan, n_dp = (mesh_shape[a] for a in ("seq", "chan", "dp"))
    _, rows, width = ssm_input.shape
    heads = step_size.shape[2]
    states = b_proj.shape[2]
    model = w_out.shape[1]
    nb = d_out.shape[2]
    half = width // 2
    chunks = max(1, min(4, half // 128))
    cw = half // chunks
    reds = 0
    for n in (n_seq, n_dp):
        while n > 1:
            reds += 1
            n //= 2
    peers = max(1, n_chan - 1)
    sizes = (n_seq, n_chan, n_dp, heads, game_lengths.shape[1], chunks)
    vmem = pl.BlockSpec(memory_space=pltpu.VMEM)
    hbm = pl.BlockSpec(memory_space=pl.ANY)
    dma = pltpu.SemaphoreType.DMA
    out, gx, gg, gs = pl.pallas_call(
        functools.partial(kernel, sizes),
        out_shape=(
            jax.ShapeDtypeStruct((rows, nb), BF16),
            jax.ShapeDtypeStruct((rows, width), BF16),
            jax.ShapeDtypeStruct((1, width), F32),
            jax.ShapeDtypeStruct((1, heads), F32),
        ),
        in_specs=[vmem] * 7 + [pl.BlockSpec(memory_space=pltpu.SMEM)] + [hbm] * 3,
        out_specs=(vmem,) * 4,
        scratch_shapes=[
            pltpu.VMEM((rows, width), BF16),
            pltpu.VMEM((width, model), BF16),
            pltpu.VMEM((n_chan, rows, nb), BF16),
            pltpu.VMEM((rows, heads), F32),
            pltpu.VMEM((heads, rows), F32),
            pltpu.VMEM((1, width), F32),
            pltpu.VMEM((1, width), F32),
            pltpu.VMEM((rows, width), F32),
            pltpu.VMEM((rows, width), F32),
            pltpu.VMEM((heads // 2, 2 * rows, rows), BF16),
            pltpu.VMEM((rows, width), F32),
            pltpu.VMEM((rows, width), F32),
            pltpu.VMEM((rows, width), F32),
            pltpu.VMEM((rows, width), BF16),
            pltpu.VMEM((rows, width), F32),
            pltpu.VMEM((rows, width), BF16),
            pltpu.VMEM((chunks, states, cw), F32),
            pltpu.VMEM((2, chunks, states, cw), BF16),
            pltpu.VMEM((2, chunks, states, cw), BF16),
            pltpu.VMEM((2, chunks, states, cw), BF16),
            pltpu.VMEM((2, chunks, states, cw), BF16),
            pltpu.VMEM((2, chunks, states, cw), BF16),
            pltpu.VMEM((2, 2 * chunks, states, cw), BF16),
            pltpu.VMEM((8, rows), F32),
            pltpu.VMEM((peers, 8, rows), F32),
            pltpu.VMEM((peers, rows, nb), BF16),
            pltpu.VMEM((peers, rows, nb), BF16),
            pltpu.VMEM((reds + 1, 2, width), F32),
            pltpu.VMEM((reds, 2, width), F32),
            dma((2,)),
            dma,
            dma((peers,)),
            dma((peers,)),
            dma((2,)),
            dma((2, chunks)),
            dma((2, chunks)),
            dma((2, chunks)),
            dma((2, chunks)),
            dma((2, chunks)),
            dma((2, chunks)),
            dma((peers,)),
            dma((peers,)),
            dma((peers,)),
            dma((peers,)),
            dma((reds,)),
            dma((reds,)),
        ],
        compiler_params=pltpu.CompilerParams(
            collective_id=0, has_side_effects=True, vmem_limit_bytes=60 * 1024 * 1024
        ),
    )(
        ssm_input[0],
        b_proj[0],
        c_proj[0],
        step_size[0],
        log_decay[0],
        skip_d[None],
        norm_gain[None],
        game_lengths,
        gate_z[0],
        w_out,
        d_out[0],
    )
    return out[None], gx[None], gg[0], gs[0]


def solution(mesh):
    return jax.shard_map(
        functools.partial(local, dict(mesh.shape)),
        mesh=mesh,
        in_specs=(
            P("dp", "seq", "chan"),
            P("dp", "seq", "chan"),
            P("dp", "seq", None),
            P("dp", "seq", None),
            P("dp", "seq", "chan"),
            P("dp", "seq", "chan"),
            P("chan"),
            P("chan"),
            P("chan", None),
            P("dp", "seq", "chan"),
            P("dp", None),
        ),
        out_specs=(P("dp", "seq", "chan"), P("dp", "seq", "chan"), P("chan"), P("chan")),
        check_vma=False,
    )
```

```python
import functools

import jax
import jax.numpy as jnp
from jax import lax
from jax.experimental import pallas as pl
from jax.experimental.pallas import tpu as pltpu
from jax.sharding import PartitionSpec as P

NORM_EPS = 1e-05
F32 = jnp.float32
BF16 = jnp.bfloat16
MESH = pl.DeviceIdType.MESH
FWD, BWD = 0, 1


def dot(a, b):
    return lax.dot_general(a, b, (((1,), (0,)), ((), ())), preferred_element_type=F32)


def dot_rows(a, b):
    return lax.dot_general(a, b, (((0,), (0,)), ((), ())), preferred_element_type=F32)


def dot_cols(a, b):
    return lax.dot_general(a, b, (((1,), (1,)), ((), ())), preferred_element_type=F32)


def split(value, terms):
    parts = []
    for _ in range(terms):
        part = value.astype(BF16)
        parts.append(part)
        value = value - part.astype(F32)
    return parts


def kernel(
    sizes,
    x_ref,
    b_ref,
    c_ref,
    dt_ref,
    ld_ref,
    skip_ref,
    gain_ref,
    gl_ref,
    z_hbm,
    w_hbm,
    do_hbm,
    out_ref,
    gx_ref,
    gg_ref,
    gs_ref,
    z_ref,
    w_ref,
    dfull,
    running_ref,
    run_row,
    decay_row,
    decay_peer,
    carry_e,
    tdt_e,
    mix_ref,
    inside_ref,
    act_ref,
    gated_ref,
    normed_ref,
    pulled_ref,
    d_ref,
    own_ref,
    tx1,
    rx1,
    txc,
    rxc,
    tx3,
    state_ref,
    stat_tx,
    stat_rx,
    proj_tx,
    proj_rx,
    proj_own,
    red_tx,
    red_rx,
    load_sem,
    dl_sem,
    do_send,
    do_recv,
    dec_sem,
    s1_send,
    s1_recv,
    sc_send,
    sc_recv,
    s3_send,
    s3_recv,
    st_send,
    st_recv,
    pj_send,
    pj_recv,
    rd_send,
    rd_recv,
):
    n_seq, n_chan, n_dp, heads, games, chunks = sizes
    rows, width = x_ref.shape
    hd = width // heads
    half = width // 2
    cw = half // chunks
    total_width = width * n_chan
    nb = out_ref.shape[1]
    seq = lax.axis_index("seq")
    chan = lax.axis_index("chan")
    dp = lax.axis_index("dp")
    mine = lax.rem(seq, 2)
    partner = {"seq": seq + 1 - 2 * mine}
    place = seq // 2
    last = n_seq // 2 - 1

    steps = []
    hop = 1
    while hop < n_dp:
        steps.append({"dp": dp + hop - 2 * hop * lax.rem(dp // hop, 2)})
        hop *= 2
    steps.append(partner)
    far = [{"seq": lax.rem(seq + 2 * k, n_seq)} for k in range(1, n_seq // 2)]
    chan_peers = [{"chan": lax.rem(chan + off, n_chan)} for off in range(1, n_chan)]
    greet = steps + chan_peers + far
    barrier = pltpu.get_barrier_semaphore()
    for peer in greet:
        pl.semaphore_signal(barrier, inc=1, device_id=peer, device_id_type=MESH)

    loads = [
        pltpu.make_async_copy(z_hbm, z_ref, load_sem.at[0]),
        pltpu.make_async_copy(w_hbm, w_ref, load_sem.at[1]),
        pltpu.make_async_copy(do_hbm, dfull.at[0], dl_sem),
    ]
    loads[2].start()
    loads[0].start()
    loads[1].start()

    def remote(src, dst, ssem, rsem, peer):
        return pltpu.make_async_remote_copy(
            src_ref=src, dst_ref=dst, send_sem=ssem, recv_sem=rsem, device_id=peer, device_id_type=MESH
        )

    row_i = lax.broadcasted_iota(jnp.int32, (rows, rows), 0)
    col_i = lax.broadcasted_iota(jnp.int32, (rows, rows), 1)
    causal = row_i >= col_i
    tri = causal.astype(F32).astype(BF16)
    running = jnp.zeros((rows, heads), F32)
    for part in split(ld_ref[...], 3):
        running = running + dot_cols(tri, part)
    running_ref[...] = running
    run_row[...] = running.T
    base = seq * rows
    count_col = jnp.zeros((rows, 1), jnp.int32)
    count_row = jnp.zeros((1, rows), jnp.int32)
    count_end = jnp.zeros((1, 1), jnp.int32)
    pos_col = base + lax.broadcasted_iota(jnp.int32, (rows, 1), 0)
    pos_row = base + lax.broadcasted_iota(jnp.int32, (1, rows), 1)
    pos_end = base + rows - 1 + lax.broadcasted_iota(jnp.int32, (1, 1), 0)
    begin = jnp.int32(0)
    for g in range(games):
        from_here = (begin >= base).astype(jnp.int32)
        count_col = count_col + (pos_col >= begin).astype(jnp.int32) * from_here
        count_row = count_row + (pos_row >= begin).astype(jnp.int32) * from_here
        count_end = count_end + (pos_end >= begin).astype(jnp.int32) * from_here
        begin = begin + gl_ref[0, g]
    end = running[rows - 1 : rows, :]
    carry = jnp.where(count_col == 0, jnp.exp(running), 0.0)
    tail = jnp.where(count_col == count_end, jnp.exp(end - running), 0.0)
    decay = jnp.where(count_end == 0, jnp.exp(end), 0.0)
    spread = (
        lax.broadcasted_iota(jnp.int32, (heads, width), 1) // hd
        == lax.broadcasted_iota(jnp.int32, (heads, width), 0)
    ).astype(F32).astype(BF16)

    def expand(value, terms):
        total = None
        for part in split(value, terms):
            piece = dot(part, spread)
            total = piece if total is None else total + piece
        return total

    tdt_e[...] = expand(tail * dt_ref[...].T, 2)
    row_pad = jnp.concatenate([decay, skip_ref[...], jnp.zeros((6, heads), F32)], axis=0)
    rows_e = expand(row_pad, 3)
    decay_row[...] = rows_e[0:1, :]
    skip_e = rows_e[1:2, :]

    group = 2 if chunks % 2 == 0 else 1
    groups = chunks // group
    gw = group * cw

    def half_cols(which, g):
        return pl.ds(pl.multiple_of(which * half + g * gw, gw), gw)

    def my_cols(c):
        return pl.ds(pl.multiple_of(mine * half + c * cw, cw), cw)

    def send1(d, c):
        return remote(tx1.at[d, c], rx1.at[d, c], s1_send.at[d, c], s1_recv.at[d, c], partner)

    def send3(d, c):
        return remote(
            tx3.at[d, c], state_ref.at[d, mine * chunks + c], s3_send.at[d, c], s3_recv.at[d, c], partner
        )

    def sendc(d, c):
        to = lax.rem(seq + (2 if d == FWD else n_seq - 2), n_seq)
        return remote(txc.at[d, c], rxc.at[d, c], sc_send.at[d, c], sc_recv.at[d, c], {"seq": to})

    has = (place > 0, place < last)
    dec = remote(decay_row, decay_peer, dec_sem.at[0], dec_sem.at[1], partner)

    def make(d, left, value_of):
        for g in range(groups):
            block = dot(left, value_of(half_cols(1 - mine, g))).astype(BF16)
            for k in range(group):
                tx1[d, g * group + k] = block[:, k * cw : (k + 1) * cw]
                send1(d, g * group + k).start()
        for g in range(groups):
            block = dot(left, value_of(half_cols(mine, g)))
            for k in range(group):
                own_ref[g * group + k] = block[:, k * cw : (k + 1) * cw]

    def chain(d):
        first = mine == (0 if d == FWD else 1)
        prev, nxt = (has[0], has[1]) if d == FWD else (has[1], has[0])

        def body(c):
            send1(d, c).wait_recv()

            @pl.when(prev)
            def _():
                sendc(d, c).wait_recv()

            @pl.when(jnp.logical_not(prev))
            def _():
                rxc[d, c] = jnp.zeros((rxc.shape[2], cw), BF16)

            dec_me = decay_row[:, my_cols(c)]
            dec_peer = decay_peer[:, my_cols(c)]
            fresh = own_ref[c]
            fresh_peer = rx1[d, c].astype(F32)
            before = rxc[d, c].astype(F32)
            after_me = dec_me * before + fresh
            after_peer = dec_peer * before + fresh_peer

            @pl.when(nxt)
            def _():
                txc[d, c] = jnp.where(
                    first, dec_peer * after_me + fresh_peer, dec_me * after_peer + fresh
                ).astype(BF16)
                sendc(d, c).start()

            tx3[d, c] = jnp.where(first, after_me, before).astype(BF16)

            @pl.when(prev)
            def _():
                send3(d, c).start()

            state_ref[d, mine * chunks + c] = jnp.where(first, before, after_peer).astype(BF16)

        for c in range(chunks):
            body(c)

        @pl.when(jnp.logical_not(prev))
        def _():
            for c in range(chunks):
                send3(d, c).start()

    pl.semaphore_wait(barrier, len(greet))
    dec.start()
    loads[2].wait()
    do_copies = []
    for k, peer in enumerate(chan_peers):
        do_copies.append(remote(dfull.at[0], dfull.at[k + 1], do_send.at[k], do_recv.at[k], peer))
        do_copies[-1].start()
    b_t = b_ref[...].T
    make(FWD, b_t, lambda cols: (tdt_e[:, cols] * x_ref[:, cols].astype(F32)).astype(BF16))

    scores = jnp.where(causal & (count_col == count_row), dot_cols(c_ref[...], b_ref[...]), 0.0)
    pos_lane = lax.broadcasted_iota(jnp.int32, (rows, 2 * hd), 1) < hd
    carry_e[...] = expand(carry, 2)
    loads[0].wait()

    def block_diag(pair):
        pair = pair.astype(F32)
        return jnp.concatenate(
            [jnp.where(pos_lane, pair, 0.0), jnp.where(pos_lane, 0.0, pair)], axis=0
        ).astype(BF16)

    for q in range(heads // 2):
        cols = slice(q * 2 * hd, (q + 1) * 2 * hd)
        mixes = []
        for h in (2 * q, 2 * q + 1):
            gap = jnp.minimum(running_ref[:, h : h + 1] - run_row[h : h + 1, :], 0.0)
            mixes.append((jnp.exp(gap) * scores * dt_ref[h : h + 1, :]).astype(BF16))
            mix_ref[q, (h % 2) * rows : (h % 2 + 1) * rows, :] = mixes[-1]
        pair = x_ref[:, cols]
        inside_ref[:, cols] = dot(jnp.concatenate(mixes, axis=1), block_diag(pair)) + skip_e[
            :, cols
        ] * pair.astype(F32)
        zf = z_ref[:, cols].astype(F32)
        act_ref[:, cols] = zf / (1.0 + jnp.exp(-zf))

    tile = min(256, width)

    def pull():
        loads[1].wait()
        for copy in do_copies:
            copy.wait_recv()

        def body(i, _):
            feats = pl.ds(pl.multiple_of(i * tile, tile), tile)
            total = None
            for k in range(n_chan):
                source = lax.rem(chan + n_chan - k, n_chan)
                piece = dot_cols(dfull[k], w_ref[feats, pl.ds(pl.multiple_of(source * nb, nb), nb)])
                total = piece if total is None else total + piece
            pulled_ref[:, feats] = total
            return 0

        lax.fori_loop(0, width // tile, body, 0)

    pl.when(place == last)(pull)
    dec.wait_recv()
    chain(FWD)
    pl.when(place < last)(pull)

    def gate(q, sums):
        squares, dots = sums
        cols = pl.ds(pl.multiple_of(q * gw, gw), gw)
        carried = jnp.concatenate(
            [dot(c_ref[...], state_ref[FWD, q * group + k]) for k in range(group)], axis=1
        )
        gated = (inside_ref[:, cols] + carry_e[:, cols] * carried) * act_ref[:, cols]
        normed = (gated * gain_ref[:, cols]).astype(BF16)
        gated_ref[:, cols] = gated
        normed_ref[:, cols] = normed
        sq = gated * gated
        od = normed.astype(F32) * pulled_ref[:, cols]
        for k in range(gw // 128):
            squares = squares + sq[:, k * 128 : (k + 1) * 128]
            dots = dots + od[:, k * 128 : (k + 1) * 128]
        return squares, dots

    zero = jnp.zeros((rows, 128), F32)
    sums = lax.fori_loop(0, groups, lambda g, s: gate(mine * groups + g, s), (zero, zero))

    def gate_late(d):
        def body(g, s):
            for k in range(group):
                send3(d, g * group + k).wait_recv()
            return gate((1 - mine) * groups + g, s)

        return body

    squares, dots = lax.fori_loop(0, groups, gate_late(FWD), sums)
    sq_col = jnp.sum(squares, axis=1, keepdims=True)
    dot_col = jnp.sum(dots, axis=1, keepdims=True)
    lane = lax.broadcasted_iota(jnp.int32, (rows, 128), 1)
    stats = jnp.where(lane == 0, sq_col, jnp.where(lane == 1, dot_col, 0.0))
    stat_tx[...] = stats.T[0:8, :]
    st_copies = []
    for k, peer in enumerate(chan_peers):
        st_copies.append(remote(stat_tx, stat_rx.at[k], st_send.at[k], st_recv.at[k], peer))
        st_copies[-1].start()
    total = stat_tx[...]
    for k, copy in enumerate(st_copies):
        copy.wait_recv()
        total = total + stat_rx[k]
    stat_cols = jnp.concatenate([total, jnp.zeros((rows - 8, rows), F32)], axis=0).T
    inv = lax.rsqrt(stat_cols[:, 0:1] / total_width + NORM_EPS)
    back = inv * inv * inv * stat_cols[:, 1:2] / total_width

    c_t = c_ref[...].T

    def cot_block(cols):
        gated = gated_ref[:, cols]
        d_normed = inv * pulled_ref[:, cols]
        d = ((gain_ref[:, cols] * d_normed - back * gated) * act_ref[:, cols]).astype(BF16)
        d_ref[:, cols] = d
        pulled_ref[:, cols] = gated * d_normed
        return (carry_e[:, cols] * d.astype(F32)).astype(BF16)

    make(BWD, c_t, cot_block)

    def cot(q, _):
        cols = pl.ds(pl.multiple_of(q * gw, gw), gw)
        red_tx[0, 0:1, cols] = jnp.sum(pulled_ref[:, cols], axis=0, keepdims=True)
        red_tx[0, 1:2, cols] = jnp.sum(
            d_ref[:, cols].astype(F32) * x_ref[:, cols].astype(F32), axis=0, keepdims=True
        )
        return 0

    lax.fori_loop(0, 2 * groups, cot, 0)

    def red(k):
        return remote(red_tx.at[k], red_rx.at[k], rd_send.at[k], rd_recv.at[k], steps[k])

    def reduce_step(k):
        red(k).wait_recv()
        red_tx[k + 1] = red_tx[k] + red_rx[k]
        if k + 1 < len(steps):
            red(k + 1).start()

    def red_far(k):
        slot = len(steps) + k
        return remote(red_tx.at[len(steps)], red_rx.at[slot], rd_send.at[slot], rd_recv.at[slot], far[k])

    red(0).start()
    tile_n = min(256, nb)

    def project(block, store):
        def body(i, _):
            at = pl.ds(pl.multiple_of(block * nb + i * tile_n, tile_n), tile_n)
            store(pl.ds(pl.multiple_of(i * tile_n, tile_n), tile_n), dot(normed_ref[...], w_ref[:, at]))
            return 0

        lax.fori_loop(0, nb // tile_n, body, 0)

    pj_copies = []
    for k, peer in enumerate(chan_peers):

        def store(at, value, k=k):
            proj_tx[k, :, at] = value.astype(BF16)

        project(peer["chan"], store)
        pj_copies.append(remote(proj_tx.at[k], proj_rx.at[k], pj_send.at[k], pj_recv.at[k], peer))
        pj_copies[-1].start()

    pl.when(place == last)(lambda: chain(BWD))
    reduce_step(0)
    def own_body(i, _):
        at = pl.ds(pl.multiple_of(chan * nb + i * tile_n, tile_n), tile_n)
        proj_own[:, pl.ds(pl.multiple_of(i * tile_n, tile_n), tile_n)] = dot(normed_ref[...], w_ref[:, at])
        return 0

    lax.fori_loop(0, nb // tile_n, own_body, 0)
    for q in range(heads // 2):
        cols = slice(q * 2 * hd, (q + 1) * 2 * hd)
        pair = d_ref[:, cols]
        inside_ref[:, cols] = dot_rows(mix_ref[q], block_diag(pair)) + skip_e[:, cols] * pair.astype(F32)

    def finish_out():
        for copy in pj_copies:
            copy.wait_recv()
        for i in range(nb // tile_n):
            at = slice(i * tile_n, (i + 1) * tile_n)
            value = proj_own[:, at]
            for k in range(n_chan - 1):
                value = value + proj_rx[k, :, at].astype(F32)
            out_ref[:, at] = (inv * value).astype(BF16)

    def settle():
        for k in range(1, len(steps)):
            reduce_step(k)
        for k in range(len(far)):
            red_far(k).start()
        finish_out()

    pl.when(place < last - 1)(settle)
    pl.when(place < last)(lambda: chain(BWD))
    pl.when(place >= last - 1)(settle)

    def finish(q):
        cols = pl.ds(pl.multiple_of(q * gw, gw), gw)
        carried = jnp.concatenate(
            [dot(b_ref[...], state_ref[BWD, q * group + k]) for k in range(group)], axis=1
        )
        gx_ref[:, cols] = (inside_ref[:, cols] + tdt_e[:, cols] * carried).astype(BF16)

    def early(g, _):
        finish(mine * groups + g)
        return 0

    def late(g, _):
        for k in range(group):
            send3(BWD, g * group + k).wait_recv()
        finish((1 - mine) * groups + g)
        return 0

    lax.fori_loop(0, groups, early, 0)
    lax.fori_loop(0, groups, late, 0)

    final = red_tx[len(steps)]
    for k in range(len(far)):
        red_far(k).wait_recv()
        final = final + red_rx[len(steps) + k]
    gg_ref[...] = final[0:1, :]
    skip_cols = jnp.concatenate([final[1:2, :], jnp.zeros((7, width), F32)], axis=0)
    skip_sum = jnp.zeros((8, heads), F32)
    for part in split(skip_cols, 3):
        skip_sum = skip_sum + dot_cols(part, spread)
    gs_ref[...] = skip_sum[0:1, :]

    dec.wait_send()
    for copy in do_copies + st_copies + pj_copies:
        copy.wait_send()
    for k in range(len(steps)):
        red(k).wait_send()
    for k in range(len(far)):
        red_far(k).wait_send()
    for d in (FWD, BWD):
        for c in range(chunks):
            send1(d, c).wait_send()
            send3(d, c).wait_send()

            @pl.when(has[1] if d == FWD else has[0])
            def _():
                sendc(d, c).wait_send()


def hand_over(*refs):
    for source, target in zip(refs[:4], refs[4:]):
        target[...] = source[...]


def local(
    mesh_shape, ssm_input, gate_z, b_proj, c_proj, step_size, log_decay, skip_d, norm_gain, w_out, d_out, game_lengths
):
    n_seq, n_chan, n_dp = (mesh_shape[a] for a in ("seq", "chan", "dp"))
    _, rows, width = ssm_input.shape
    heads = step_size.shape[2]
    states = b_proj.shape[2]
    model = w_out.shape[1]
    nb = d_out.shape[2]
    half = width // 2
    chunks = max(1, min(8, half // 128))
    cw = half // chunks
    reds = n_dp.bit_length()
    slots = reds + n_seq // 2 - 1
    peers = max(1, n_chan - 1)
    sizes = (n_seq, n_chan, n_dp, heads, game_lengths.shape[1], chunks)
    vmem = pl.BlockSpec(memory_space=pltpu.VMEM)
    hbm = pl.BlockSpec(memory_space=pltpu.HBM)
    dma = pltpu.SemaphoreType.DMA
    out, gx, gg, gs = pl.pallas_call(
        functools.partial(kernel, sizes),
        out_shape=(
            jax.ShapeDtypeStruct((rows, nb), BF16),
            jax.ShapeDtypeStruct((rows, width), BF16),
            jax.ShapeDtypeStruct((1, width), F32),
            jax.ShapeDtypeStruct((1, heads), F32),
        ),
        in_specs=[vmem] * 7 + [pl.BlockSpec(memory_space=pltpu.SMEM)] + [hbm] * 3,
        out_specs=(vmem,) * 4,
        scratch_shapes=[
            pltpu.VMEM((rows, width), BF16),
            pltpu.VMEM((width, model), BF16),
            pltpu.VMEM((n_chan, rows, nb), BF16),
            pltpu.VMEM((rows, heads), F32),
            pltpu.VMEM((heads, rows), F32),
            pltpu.VMEM((1, width), F32),
            pltpu.VMEM((1, width), F32),
            pltpu.VMEM((rows, width), F32),
            pltpu.VMEM((rows, width), F32),
            pltpu.VMEM((heads // 2, 2 * rows, rows), BF16),
            pltpu.VMEM((rows, width), F32),
            pltpu.VMEM((rows, width), F32),
            pltpu.VMEM((rows, width), F32),
            pltpu.VMEM((rows, width), BF16),
            pltpu.VMEM((rows, width), F32),
            pltpu.VMEM((rows, width), BF16),
            pltpu.VMEM((chunks, states, cw), F32),
            pltpu.VMEM((2, chunks, states, cw), BF16),
            pltpu.VMEM((2, chunks, states, cw), BF16),
            pltpu.VMEM((2, chunks, states, cw), BF16),
            pltpu.VMEM((2, chunks, states, cw), BF16),
            pltpu.VMEM((2, chunks, states, cw), BF16),
            pltpu.VMEM((2, 2 * chunks, states, cw), BF16),
            pltpu.VMEM((8, rows), F32),
            pltpu.VMEM((peers, 8, rows), F32),
            pltpu.VMEM((peers, rows, nb), BF16),
            pltpu.VMEM((peers, rows, nb), BF16),
            pltpu.VMEM((rows, nb), F32),
            pltpu.VMEM((reds + 1, 2, width), F32),
            pltpu.VMEM((slots, 2, width), F32),
            dma((2,)),
            dma,
            dma((peers,)),
            dma((peers,)),
            dma((2,)),
            dma((2, chunks)),
            dma((2, chunks)),
            dma((2, chunks)),
            dma((2, chunks)),
            dma((2, chunks)),
            dma((2, chunks)),
            dma((peers,)),
            dma((peers,)),
            dma((peers,)),
            dma((peers,)),
            dma((slots,)),
            dma((slots,)),
        ],
        compiler_params=pltpu.CompilerParams(
            collective_id=0, has_side_effects=True, vmem_limit_bytes=60 * 1024 * 1024
        ),
    )(
        ssm_input[0],
        b_proj[0],
        c_proj[0],
        step_size[0].T,
        log_decay[0].T,
        skip_d[None],
        norm_gain[None],
        game_lengths,
        gate_z[0],
        w_out,
        d_out[0],
    )
    results = (out, gx, gg, gs)
    out, gx, gg, gs = pl.pallas_call(
        hand_over,
        out_shape=tuple(jax.ShapeDtypeStruct(a.shape, a.dtype) for a in results),
        in_specs=[vmem] * 4,
        out_specs=(vmem,) * 4,
    )(*results)
    return out[None], gx[None], gg[0], gs[0]


def solution(mesh):
    return jax.shard_map(
        functools.partial(local, dict(mesh.shape)),
        mesh=mesh,
        in_specs=(
            P("dp", "seq", "chan"),
            P("dp", "seq", "chan"),
            P("dp", "seq", None),
            P("dp", "seq", None),
            P("dp", "seq", "chan"),
            P("dp", "seq", "chan"),
            P("chan"),
            P("chan"),
            P("chan", None),
            P("dp", "seq", "chan"),
            P("dp", None),
        ),
        out_specs=(P("dp", "seq", "chan"), P("dp", "seq", "chan"), P("chan"), P("chan")),
        check_vma=False,
    )
```

```python
import functools

import jax
import jax.numpy as jnp
from jax import lax
from jax.experimental import pallas as pl
from jax.experimental.pallas import tpu as pltpu
from jax.sharding import PartitionSpec as P

NORM_EPS = 1e-05
F32 = jnp.float32
BF16 = jnp.bfloat16
MESH = pl.DeviceIdType.MESH
FWD, BWD = 0, 1


def dot(a, b):
    return lax.dot_general(a, b, (((1,), (0,)), ((), ())), preferred_element_type=F32)


def dot_rows(a, b):
    return lax.dot_general(a, b, (((0,), (0,)), ((), ())), preferred_element_type=F32)


def dot_cols(a, b):
    return lax.dot_general(a, b, (((1,), (1,)), ((), ())), preferred_element_type=F32)


def split(value, terms):
    parts = []
    for _ in range(terms):
        part = value.astype(BF16)
        parts.append(part)
        value = value - part.astype(F32)
    return parts


def kernel(
    sizes,
    x_ref,
    b_ref,
    c_ref,
    dt_ref,
    ld_ref,
    skip_ref,
    gain_ref,
    gl_ref,
    z_hbm,
    w_hbm,
    do_hbm,
    out_ref,
    gx_ref,
    gg_ref,
    gs_ref,
    z_ref,
    w_ref,
    dfull,
    running_ref,
    run_row,
    decay_row,
    decay_peer,
    carry_e,
    tdt_e,
    mix_ref,
    inside_ref,
    act_ref,
    gated_ref,
    normed_ref,
    pulled_ref,
    d_ref,
    own_ref,
    tx1,
    rx1,
    txc,
    rxc,
    tx3,
    state_ref,
    stat_tx,
    stat_rx,
    proj_tx,
    proj_rx,
    proj_own,
    red_tx,
    red_rx,
    load_sem,
    dl_sem,
    do_send,
    do_recv,
    dec_sem,
    s1_send,
    s1_recv,
    sc_send,
    sc_recv,
    s3_send,
    s3_recv,
    st_send,
    st_recv,
    pj_send,
    pj_recv,
    rd_send,
    rd_recv,
):
    n_seq, n_chan, n_dp, heads, games, chunks = sizes
    rows, width = x_ref.shape
    hd = width // heads
    half = width // 2
    cw = half // chunks
    total_width = width * n_chan
    nb = out_ref.shape[1]
    seq = lax.axis_index("seq")
    chan = lax.axis_index("chan")
    dp = lax.axis_index("dp")
    mine = lax.rem(seq, 2)
    partner = {"seq": seq + 1 - 2 * mine}
    place = seq // 2
    last = n_seq // 2 - 1

    steps = []
    hop = 1
    while hop < n_dp:
        steps.append({"dp": dp + hop - 2 * hop * lax.rem(dp // hop, 2)})
        hop *= 2
    steps.append(partner)
    far = [{"seq": lax.rem(seq + 2 * k, n_seq)} for k in range(1, n_seq // 2)]
    chan_peers = [{"chan": lax.rem(chan + off, n_chan)} for off in range(1, n_chan)]
    greet = steps + chan_peers + far
    barrier = pltpu.get_barrier_semaphore()
    for peer in greet:
        pl.semaphore_signal(barrier, inc=1, device_id=peer, device_id_type=MESH)

    loads = [
        pltpu.make_async_copy(z_hbm, z_ref, load_sem.at[0]),
        pltpu.make_async_copy(w_hbm, w_ref, load_sem.at[1]),
        pltpu.make_async_copy(do_hbm, dfull.at[0], dl_sem),
    ]
    loads[2].start()
    loads[0].start()
    loads[1].start()

    def remote(src, dst, ssem, rsem, peer):
        return pltpu.make_async_remote_copy(
            src_ref=src, dst_ref=dst, send_sem=ssem, recv_sem=rsem, device_id=peer, device_id_type=MESH
        )

    row_i = lax.broadcasted_iota(jnp.int32, (rows, rows), 0)
    col_i = lax.broadcasted_iota(jnp.int32, (rows, rows), 1)
    causal = row_i >= col_i
    tri = causal.astype(F32).astype(BF16)
    running = jnp.zeros((rows, heads), F32)
    for part in split(ld_ref[...], 3):
        running = running + dot_cols(tri, part)
    running_ref[...] = running
    run_row[...] = running.T
    base = seq * rows
    count_col = jnp.zeros((rows, 1), jnp.int32)
    count_row = jnp.zeros((1, rows), jnp.int32)
    count_end = jnp.zeros((1, 1), jnp.int32)
    pos_col = base + lax.broadcasted_iota(jnp.int32, (rows, 1), 0)
    pos_row = base + lax.broadcasted_iota(jnp.int32, (1, rows), 1)
    pos_end = base + rows - 1 + lax.broadcasted_iota(jnp.int32, (1, 1), 0)
    begin = jnp.int32(0)
    for g in range(games):
        from_here = (begin >= base).astype(jnp.int32)
        count_col = count_col + (pos_col >= begin).astype(jnp.int32) * from_here
        count_row = count_row + (pos_row >= begin).astype(jnp.int32) * from_here
        count_end = count_end + (pos_end >= begin).astype(jnp.int32) * from_here
        begin = begin + gl_ref[0, g]
    end = running[rows - 1 : rows, :]
    carry = jnp.where(count_col == 0, jnp.exp(running), 0.0)
    tail = jnp.where(count_col == count_end, jnp.exp(end - running), 0.0)
    decay = jnp.where(count_end == 0, jnp.exp(end), 0.0)
    spread = (
        lax.broadcasted_iota(jnp.int32, (heads, width), 1) // hd
        == lax.broadcasted_iota(jnp.int32, (heads, width), 0)
    ).astype(F32).astype(BF16)

    def expand(value, terms):
        total = None
        for part in split(value, terms):
            piece = dot(part, spread)
            total = piece if total is None else total + piece
        return total

    tdt_e[...] = expand(tail * dt_ref[...].T, 2)
    row_pad = jnp.concatenate([decay, skip_ref[...], jnp.zeros((6, heads), F32)], axis=0)
    rows_e = expand(row_pad, 3)
    decay_row[...] = rows_e[0:1, :]
    skip_e = rows_e[1:2, :]

    group = 2 if chunks % 2 == 0 else 1
    groups = chunks // group
    gw = group * cw

    def half_cols(which, g):
        return pl.ds(pl.multiple_of(which * half + g * gw, gw), gw)

    def my_cols(c):
        return pl.ds(pl.multiple_of(mine * half + c * cw, cw), cw)

    def send1(d, c):
        return remote(tx1.at[d, c], rx1.at[d, c], s1_send.at[d, c], s1_recv.at[d, c], partner)

    def send3(d, c):
        return remote(
            tx3.at[d, c], state_ref.at[d, mine * chunks + c], s3_send.at[d, c], s3_recv.at[d, c], partner
        )

    def sendc(d, c):
        to = lax.rem(seq + (2 if d == FWD else n_seq - 2), n_seq)
        return remote(txc.at[d, c], rxc.at[d, c], sc_send.at[d, c], sc_recv.at[d, c], {"seq": to})

    has = (place > 0, place < last)
    dec = remote(decay_row, decay_peer, dec_sem.at[0], dec_sem.at[1], partner)

    def make(d, left, value_of):
        for g in range(groups):
            block = dot(left, value_of(half_cols(1 - mine, g))).astype(BF16)
            for k in range(group):
                tx1[d, g * group + k] = block[:, k * cw : (k + 1) * cw]
                send1(d, g * group + k).start()
        for g in range(groups):
            block = dot(left, value_of(half_cols(mine, g)))
            for k in range(group):
                own_ref[g * group + k] = block[:, k * cw : (k + 1) * cw]

    def chain(d):
        first = mine == (0 if d == FWD else 1)
        prev, nxt = (has[0], has[1]) if d == FWD else (has[1], has[0])

        def body(c):
            send1(d, c).wait_recv()

            @pl.when(prev)
            def _():
                sendc(d, c).wait_recv()

            @pl.when(jnp.logical_not(prev))
            def _():
                rxc[d, c] = jnp.zeros((rxc.shape[2], cw), BF16)

            dec_me = decay_row[:, my_cols(c)]
            dec_peer = decay_peer[:, my_cols(c)]
            fresh = own_ref[c]
            fresh_peer = rx1[d, c].astype(F32)
            before = rxc[d, c].astype(F32)
            after_me = dec_me * before + fresh
            after_peer = dec_peer * before + fresh_peer

            @pl.when(nxt)
            def _():
                txc[d, c] = jnp.where(
                    first, dec_peer * after_me + fresh_peer, dec_me * after_peer + fresh
                ).astype(BF16)
                sendc(d, c).start()

            tx3[d, c] = jnp.where(first, after_me, before).astype(BF16)

            @pl.when(prev)
            def _():
                send3(d, c).start()

            state_ref[d, mine * chunks + c] = jnp.where(first, before, after_peer).astype(BF16)

        for c in range(chunks):
            body(c)

    def head_sends(d):
        for c in range(chunks):
            send3(d, c).start()

    pl.semaphore_wait(barrier, len(greet))
    dec.start()
    loads[2].wait()
    do_copies = []
    for k, peer in enumerate(chan_peers):
        do_copies.append(remote(dfull.at[0], dfull.at[k + 1], do_send.at[k], do_recv.at[k], peer))
        do_copies[-1].start()
    b_t = b_ref[...].T
    make(FWD, b_t, lambda cols: (tdt_e[:, cols] * x_ref[:, cols].astype(F32)).astype(BF16))

    scores = jnp.where(causal & (count_col == count_row), dot_cols(c_ref[...], b_ref[...]), 0.0)
    pos_lane = lax.broadcasted_iota(jnp.int32, (rows, 2 * hd), 1) < hd
    carry_e[...] = expand(carry, 2)
    loads[0].wait()

    def block_diag(pair):
        pair = pair.astype(F32)
        return jnp.concatenate(
            [jnp.where(pos_lane, pair, 0.0), jnp.where(pos_lane, 0.0, pair)], axis=0
        ).astype(BF16)

    for q in range(heads // 2):
        cols = slice(q * 2 * hd, (q + 1) * 2 * hd)
        mixes = []
        for h in (2 * q, 2 * q + 1):
            gap = jnp.minimum(running_ref[:, h : h + 1] - run_row[h : h + 1, :], 0.0)
            mixes.append((jnp.exp(gap) * scores * dt_ref[h : h + 1, :]).astype(BF16))
            mix_ref[q, (h % 2) * rows : (h % 2 + 1) * rows, :] = mixes[-1]
        pair = x_ref[:, cols]
        inside_ref[:, cols] = dot(jnp.concatenate(mixes, axis=1), block_diag(pair)) + skip_e[
            :, cols
        ] * pair.astype(F32)
        zf = z_ref[:, cols].astype(F32)
        act_ref[:, cols] = zf / (1.0 + jnp.exp(-zf))

    tile = min(256, width)

    def pull():
        loads[1].wait()
        for copy in do_copies:
            copy.wait_recv()

        def body(i, _):
            feats = pl.ds(pl.multiple_of(i * tile, tile), tile)
            total = None
            for k in range(n_chan):
                source = lax.rem(chan + n_chan - k, n_chan)
                piece = dot_cols(dfull[k], w_ref[feats, pl.ds(pl.multiple_of(source * nb, nb), nb)])
                total = piece if total is None else total + piece
            pulled_ref[:, feats] = total
            return 0

        lax.fori_loop(0, width // tile, body, 0)

    pl.when(place == last)(pull)
    dec.wait_recv()
    chain(FWD)
    pl.when(place == 0)(lambda: head_sends(FWD))
    pl.when(place < last)(pull)

    def gate(q, sums):
        squares, dots = sums
        cols = pl.ds(pl.multiple_of(q * gw, gw), gw)
        carried = jnp.concatenate(
            [dot(c_ref[...], state_ref[FWD, q * group + k]) for k in range(group)], axis=1
        )
        gated = (inside_ref[:, cols] + carry_e[:, cols] * carried) * act_ref[:, cols]
        normed = (gated * gain_ref[:, cols]).astype(BF16)
        gated_ref[:, cols] = gated
        normed_ref[:, cols] = normed
        sq = gated * gated
        od = normed.astype(F32) * pulled_ref[:, cols]
        for k in range(gw // 128):
            squares = squares + sq[:, k * 128 : (k + 1) * 128]
            dots = dots + od[:, k * 128 : (k + 1) * 128]
        return squares, dots

    zero = jnp.zeros((rows, 128), F32)
    sums = lax.fori_loop(0, groups, lambda g, s: gate(mine * groups + g, s), (zero, zero))

    def gate_late(d):
        def body(g, s):
            for k in range(group):
                send3(d, g * group + k).wait_recv()
            return gate((1 - mine) * groups + g, s)

        return body

    squares, dots = lax.fori_loop(0, groups, gate_late(FWD), sums)
    sq_col = jnp.sum(squares, axis=1, keepdims=True)
    dot_col = jnp.sum(dots, axis=1, keepdims=True)
    lane = lax.broadcasted_iota(jnp.int32, (rows, 128), 1)
    stats = jnp.where(lane == 0, sq_col, jnp.where(lane == 1, dot_col, 0.0))
    stat_tx[...] = stats.T[0:8, :]
    st_copies = []
    for k, peer in enumerate(chan_peers):
        st_copies.append(remote(stat_tx, stat_rx.at[k], st_send.at[k], st_recv.at[k], peer))
        st_copies[-1].start()
    total = stat_tx[...]
    for k, copy in enumerate(st_copies):
        copy.wait_recv()
        total = total + stat_rx[k]
    stat_cols = jnp.concatenate([total, jnp.zeros((rows - 8, rows), F32)], axis=0).T
    inv = lax.rsqrt(stat_cols[:, 0:1] / total_width + NORM_EPS)
    back = inv * inv * inv * stat_cols[:, 1:2] / total_width

    c_t = c_ref[...].T

    def cot_block(cols):
        gated = gated_ref[:, cols]
        d_normed = inv * pulled_ref[:, cols]
        d = ((gain_ref[:, cols] * d_normed - back * gated) * act_ref[:, cols]).astype(BF16)
        d_ref[:, cols] = d
        pulled_ref[:, cols] = gated * d_normed
        return (carry_e[:, cols] * d.astype(F32)).astype(BF16)

    make(BWD, c_t, cot_block)

    def cot(q, _):
        cols = pl.ds(pl.multiple_of(q * gw, gw), gw)
        red_tx[0, 0:1, cols] = jnp.sum(pulled_ref[:, cols], axis=0, keepdims=True)
        red_tx[0, 1:2, cols] = jnp.sum(
            d_ref[:, cols].astype(F32) * x_ref[:, cols].astype(F32), axis=0, keepdims=True
        )
        return 0

    lax.fori_loop(0, 2 * groups, cot, 0)

    def red(k):
        return remote(red_tx.at[k], red_rx.at[k], rd_send.at[k], rd_recv.at[k], steps[k])

    def reduce_step(k):
        red(k).wait_recv()
        red_tx[k + 1] = red_tx[k] + red_rx[k]
        if k + 1 < len(steps):
            red(k + 1).start()

    def red_far(k):
        slot = len(steps) + k
        return remote(red_tx.at[len(steps)], red_rx.at[slot], rd_send.at[slot], rd_recv.at[slot], far[k])

    red(0).start()
    tile_n = min(256, nb)

    def project(block, store):
        def body(i, _):
            at = pl.ds(pl.multiple_of(block * nb + i * tile_n, tile_n), tile_n)
            store(pl.ds(pl.multiple_of(i * tile_n, tile_n), tile_n), dot(normed_ref[...], w_ref[:, at]))
            return 0

        lax.fori_loop(0, nb // tile_n, body, 0)

    pj_copies = []
    for k, peer in enumerate(chan_peers):

        def store(at, value, k=k):
            proj_tx[k, :, at] = value.astype(BF16)

        project(peer["chan"], store)
        pj_copies.append(remote(proj_tx.at[k], proj_rx.at[k], pj_send.at[k], pj_recv.at[k], peer))
        pj_copies[-1].start()

    pl.when(place == last)(lambda: chain(BWD))
    reduce_step(0)
    def own_body(i, _):
        at = pl.ds(pl.multiple_of(chan * nb + i * tile_n, tile_n), tile_n)
        proj_own[:, pl.ds(pl.multiple_of(i * tile_n, tile_n), tile_n)] = dot(normed_ref[...], w_ref[:, at])
        return 0

    lax.fori_loop(0, nb // tile_n, own_body, 0)
    for q in range(heads // 2):
        cols = slice(q * 2 * hd, (q + 1) * 2 * hd)
        pair = d_ref[:, cols]
        inside_ref[:, cols] = dot_rows(mix_ref[q], block_diag(pair)) + skip_e[:, cols] * pair.astype(F32)

    def finish_out():
        for copy in pj_copies:
            copy.wait_recv()
        for i in range(nb // tile_n):
            at = slice(i * tile_n, (i + 1) * tile_n)
            value = proj_own[:, at]
            for k in range(n_chan - 1):
                value = value + proj_rx[k, :, at].astype(F32)
            out_ref[:, at] = (inv * value).astype(BF16)

    def settle():
        for k in range(1, len(steps)):
            reduce_step(k)
        for k in range(len(far)):
            red_far(k).start()
        finish_out()

    pl.when(place < last - 1)(settle)
    pl.when(place < last)(lambda: chain(BWD))
    pl.when(place >= last - 1)(settle)
    pl.when(place == last)(lambda: head_sends(BWD))

    def finish(q):
        cols = pl.ds(pl.multiple_of(q * gw, gw), gw)
        carried = jnp.concatenate(
            [dot(b_ref[...], state_ref[BWD, q * group + k]) for k in range(group)], axis=1
        )
        gx_ref[:, cols] = (inside_ref[:, cols] + tdt_e[:, cols] * carried).astype(BF16)

    def early(g, _):
        finish(mine * groups + g)
        return 0

    def late(g, _):
        for k in range(group):
            send3(BWD, g * group + k).wait_recv()
        finish((1 - mine) * groups + g)
        return 0

    lax.fori_loop(0, groups, early, 0)
    lax.fori_loop(0, groups, late, 0)

    final = red_tx[len(steps)]
    for k in range(len(far)):
        red_far(k).wait_recv()
        final = final + red_rx[len(steps) + k]
    gg_ref[...] = final[0:1, :]
    skip_cols = jnp.concatenate([final[1:2, :], jnp.zeros((7, width), F32)], axis=0)
    skip_sum = jnp.zeros((8, heads), F32)
    for part in split(skip_cols, 3):
        skip_sum = skip_sum + dot_cols(part, spread)
    gs_ref[...] = skip_sum[0:1, :]

    dec.wait_send()
    for copy in do_copies + st_copies + pj_copies:
        copy.wait_send()
    for k in range(len(steps)):
        red(k).wait_send()
    for k in range(len(far)):
        red_far(k).wait_send()
    for d in (FWD, BWD):
        for c in range(chunks):
            send1(d, c).wait_send()
            send3(d, c).wait_send()

            @pl.when(has[1] if d == FWD else has[0])
            def _():
                sendc(d, c).wait_send()


def hand_over(*refs):
    for source, target in zip(refs[:4], refs[4:]):
        target[...] = source[...]


def local(
    mesh_shape, ssm_input, gate_z, b_proj, c_proj, step_size, log_decay, skip_d, norm_gain, w_out, d_out, game_lengths
):
    n_seq, n_chan, n_dp = (mesh_shape[a] for a in ("seq", "chan", "dp"))
    _, rows, width = ssm_input.shape
    heads = step_size.shape[2]
    states = b_proj.shape[2]
    model = w_out.shape[1]
    nb = d_out.shape[2]
    half = width // 2
    chunks = max(1, min(8, half // 128))
    cw = half // chunks
    reds = n_dp.bit_length()
    slots = reds + n_seq // 2 - 1
    peers = max(1, n_chan - 1)
    sizes = (n_seq, n_chan, n_dp, heads, game_lengths.shape[1], chunks)
    vmem = pl.BlockSpec(memory_space=pltpu.VMEM)
    hbm = pl.BlockSpec(memory_space=pltpu.HBM)
    dma = pltpu.SemaphoreType.DMA
    out, gx, gg, gs = pl.pallas_call(
        functools.partial(kernel, sizes),
        out_shape=(
            pltpu.VMEM((rows, nb), BF16),
            pltpu.VMEM((rows, width), BF16),
            pltpu.VMEM((1, width), F32),
            pltpu.VMEM((1, heads), F32),
        ),
        in_specs=[vmem] * 7 + [pl.BlockSpec(memory_space=pltpu.SMEM)] + [hbm] * 3,
        out_specs=(vmem,) * 4,
        scratch_shapes=[
            pltpu.VMEM((rows, width), BF16),
            pltpu.VMEM((width, model), BF16),
            pltpu.VMEM((n_chan, rows, nb), BF16),
            pltpu.VMEM((rows, heads), F32),
            pltpu.VMEM((heads, rows), F32),
            pltpu.VMEM((1, width), F32),
            pltpu.VMEM((1, width), F32),
            pltpu.VMEM((rows, width), F32),
            pltpu.VMEM((rows, width), F32),
            pltpu.VMEM((heads // 2, 2 * rows, rows), BF16),
            pltpu.VMEM((rows, width), F32),
            pltpu.VMEM((rows, width), F32),
            pltpu.VMEM((rows, width), F32),
            pltpu.VMEM((rows, width), BF16),
            pltpu.VMEM((rows, width), F32),
            pltpu.VMEM((rows, width), BF16),
            pltpu.VMEM((chunks, states, cw), F32),
            pltpu.VMEM((2, chunks, states, cw), BF16),
            pltpu.VMEM((2, chunks, states, cw), BF16),
            pltpu.VMEM((2, chunks, states, cw), BF16),
            pltpu.VMEM((2, chunks, states, cw), BF16),
            pltpu.VMEM((2, chunks, states, cw), BF16),
            pltpu.VMEM((2, 2 * chunks, states, cw), BF16),
            pltpu.VMEM((8, rows), F32),
            pltpu.VMEM((peers, 8, rows), F32),
            pltpu.VMEM((peers, rows, nb), BF16),
            pltpu.VMEM((peers, rows, nb), BF16),
            pltpu.VMEM((rows, nb), F32),
            pltpu.VMEM((reds + 1, 2, width), F32),
            pltpu.VMEM((slots, 2, width), F32),
            dma((2,)),
            dma,
            dma((peers,)),
            dma((peers,)),
            dma((2,)),
            dma((2, chunks)),
            dma((2, chunks)),
            dma((2, chunks)),
            dma((2, chunks)),
            dma((2, chunks)),
            dma((2, chunks)),
            dma((peers,)),
            dma((peers,)),
            dma((peers,)),
            dma((peers,)),
            dma((slots,)),
            dma((slots,)),
        ],
        compiler_params=pltpu.CompilerParams(
            collective_id=0, has_side_effects=True, vmem_limit_bytes=60 * 1024 * 1024
        ),
    )(
        ssm_input[0],
        b_proj[0],
        c_proj[0],
        step_size[0].T,
        log_decay[0].T,
        skip_d[None],
        norm_gain[None],
        game_lengths,
        gate_z[0],
        w_out,
        d_out[0],
    )
    results = (out, gx, gg, gs)
    out, gx, gg, gs = pl.pallas_call(
        hand_over,
        out_shape=tuple(jax.ShapeDtypeStruct(a.shape, a.dtype) for a in results),
        in_specs=[vmem] * 4,
        out_specs=(vmem,) * 4,
        compiler_params=pltpu.CompilerParams(vmem_limit_bytes=4 * 1024 * 1024),
    )(*results)
    return out[None], gx[None], gg[0], gs[0]


def solution(mesh):
    return jax.shard_map(
        functools.partial(local, dict(mesh.shape)),
        mesh=mesh,
        in_specs=(
            P("dp", "seq", "chan"),
            P("dp", "seq", "chan"),
            P("dp", "seq", None),
            P("dp", "seq", None),
            P("dp", "seq", "chan"),
            P("dp", "seq", "chan"),
            P("chan"),
            P("chan"),
            P("chan", None),
            P("dp", "seq", "chan"),
            P("dp", None),
        ),
        out_specs=(P("dp", "seq", "chan"), P("dp", "seq", "chan"), P("chan"), P("chan")),
        check_vma=False,
    )
```

```python
import functools

import jax
import jax.numpy as jnp
from jax import lax
from jax.experimental import pallas as pl
from jax.experimental.pallas import tpu as pltpu
from jax.sharding import PartitionSpec as P

NORM_EPS = 1e-05
F32 = jnp.float32
BF16 = jnp.bfloat16
MESH = pl.DeviceIdType.MESH
FWD, BWD = 0, 1


def dot(a, b):
    return lax.dot_general(a, b, (((1,), (0,)), ((), ())), preferred_element_type=F32)


def dot_rows(a, b):
    return lax.dot_general(a, b, (((0,), (0,)), ((), ())), preferred_element_type=F32)


def dot_cols(a, b):
    return lax.dot_general(a, b, (((1,), (1,)), ((), ())), preferred_element_type=F32)


def split(value, terms):
    parts = []
    for _ in range(terms):
        part = value.astype(BF16)
        parts.append(part)
        value = value - part.astype(F32)
    return parts


def kernel(
    sizes,
    x_hbm,
    b_ref,
    c_ref,
    dt_ref,
    ld_ref,
    skip_ref,
    gain_ref,
    gl_ref,
    z_hbm,
    w_hbm,
    do_hbm,
    out_ref,
    gx_ref,
    gg_ref,
    gs_ref,
    x_ref,
    z_ref,
    w_ref,
    dfull,
    running_ref,
    run_row,
    decay_row,
    decay_peer,
    carry_e,
    tdt_e,
    mix_ref,
    inside_ref,
    act_ref,
    gated_ref,
    normed_ref,
    pulled_ref,
    d_ref,
    own_ref,
    tx1,
    rx1,
    txc,
    rxc,
    tx3,
    state_ref,
    stat_tx,
    stat_rx,
    proj_tx,
    proj_rx,
    proj_own,
    red_tx,
    red_rx,
    load_sem,
    dl_sem,
    do_send,
    do_recv,
    dec_sem,
    s1_send,
    s1_recv,
    sc_send,
    sc_recv,
    s3_send,
    s3_recv,
    st_send,
    st_recv,
    pj_send,
    pj_recv,
    rd_send,
    rd_recv,
):
    n_seq, n_chan, n_dp, heads, games, chunks = sizes
    rows, width = x_ref.shape
    hd = width // heads
    half = width // 2
    cw = half // chunks
    total_width = width * n_chan
    nb = out_ref.shape[1]
    seq = lax.axis_index("seq")
    chan = lax.axis_index("chan")
    dp = lax.axis_index("dp")
    mine = lax.rem(seq, 2)
    partner = {"seq": seq + 1 - 2 * mine}
    place = seq // 2
    last = n_seq // 2 - 1

    steps = []
    hop = 1
    while hop < n_dp:
        steps.append({"dp": dp + hop - 2 * hop * lax.rem(dp // hop, 2)})
        hop *= 2
    steps.append(partner)
    far = [{"seq": lax.rem(seq + 2 * k, n_seq)} for k in range(1, n_seq // 2)]
    chan_peers = [{"chan": lax.rem(chan + off, n_chan)} for off in range(1, n_chan)]
    greet = steps + chan_peers + far
    barrier = pltpu.get_barrier_semaphore()
    for peer in greet:
        pl.semaphore_signal(barrier, inc=1, device_id=peer, device_id_type=MESH)

    loads = [
        pltpu.make_async_copy(z_hbm, z_ref, load_sem.at[0]),
        pltpu.make_async_copy(w_hbm, w_ref, load_sem.at[1]),
        pltpu.make_async_copy(do_hbm, dfull.at[0], dl_sem),
    ]
    load_x = pltpu.make_async_copy(x_hbm, x_ref, load_sem.at[2])
    load_x.start()
    loads[2].start()
    loads[0].start()
    loads[1].start()

    def remote(src, dst, ssem, rsem, peer):
        return pltpu.make_async_remote_copy(
            src_ref=src, dst_ref=dst, send_sem=ssem, recv_sem=rsem, device_id=peer, device_id_type=MESH
        )

    row_i = lax.broadcasted_iota(jnp.int32, (rows, rows), 0)
    col_i = lax.broadcasted_iota(jnp.int32, (rows, rows), 1)
    causal = row_i >= col_i
    tri = causal.astype(F32).astype(BF16)
    running = jnp.zeros((rows, heads), F32)
    for part in split(ld_ref[...], 3):
        running = running + dot_cols(tri, part)
    running_ref[...] = running
    run_row[...] = running.T
    base = seq * rows
    count_col = jnp.zeros((rows, 1), jnp.int32)
    count_row = jnp.zeros((1, rows), jnp.int32)
    count_end = jnp.zeros((1, 1), jnp.int32)
    pos_col = base + lax.broadcasted_iota(jnp.int32, (rows, 1), 0)
    pos_row = base + lax.broadcasted_iota(jnp.int32, (1, rows), 1)
    pos_end = base + rows - 1 + lax.broadcasted_iota(jnp.int32, (1, 1), 0)
    begin = jnp.int32(0)
    for g in range(games):
        from_here = (begin >= base).astype(jnp.int32)
        count_col = count_col + (pos_col >= begin).astype(jnp.int32) * from_here
        count_row = count_row + (pos_row >= begin).astype(jnp.int32) * from_here
        count_end = count_end + (pos_end >= begin).astype(jnp.int32) * from_here
        begin = begin + gl_ref[0, g]
    end = running[rows - 1 : rows, :]
    carry = jnp.where(count_col == 0, jnp.exp(running), 0.0)
    tail = jnp.where(count_col == count_end, jnp.exp(end - running), 0.0)
    decay = jnp.where(count_end == 0, jnp.exp(end), 0.0)
    spread = (
        lax.broadcasted_iota(jnp.int32, (heads, width), 1) // hd
        == lax.broadcasted_iota(jnp.int32, (heads, width), 0)
    ).astype(F32).astype(BF16)

    def expand(value, terms):
        total = None
        for part in split(value, terms):
            piece = dot(part, spread)
            total = piece if total is None else total + piece
        return total

    tdt_e[...] = expand(tail * dt_ref[...].T, 2)
    row_pad = jnp.concatenate([decay, skip_ref[...], jnp.zeros((6, heads), F32)], axis=0)
    rows_e = expand(row_pad, 3)
    decay_row[...] = rows_e[0:1, :]
    skip_e = rows_e[1:2, :]

    group = 2 if chunks % 2 == 0 else 1
    groups = chunks // group
    gw = group * cw

    def half_cols(which, g):
        return pl.ds(pl.multiple_of(which * half + g * gw, gw), gw)

    def my_cols(c):
        return pl.ds(pl.multiple_of(mine * half + c * cw, cw), cw)

    def send1(d, c):
        return remote(tx1.at[d, c], rx1.at[d, c], s1_send.at[d, c], s1_recv.at[d, c], partner)

    def send3(d, c):
        return remote(
            tx3.at[d, c], state_ref.at[d, mine * chunks + c], s3_send.at[d, c], s3_recv.at[d, c], partner
        )

    def sendc(d, c):
        to = lax.rem(seq + (2 if d == FWD else n_seq - 2), n_seq)
        return remote(txc.at[d, c], rxc.at[d, c], sc_send.at[d, c], sc_recv.at[d, c], {"seq": to})

    has = (place > 0, place < last)
    dec = remote(decay_row, decay_peer, dec_sem.at[0], dec_sem.at[1], partner)

    def make(d, left, value_of):
        for g in range(groups):
            block = dot(left, value_of(half_cols(1 - mine, g))).astype(BF16)
            for k in range(group):
                tx1[d, g * group + k] = block[:, k * cw : (k + 1) * cw]
                send1(d, g * group + k).start()
        for g in range(groups):
            block = dot(left, value_of(half_cols(mine, g)))
            for k in range(group):
                own_ref[g * group + k] = block[:, k * cw : (k + 1) * cw]

    def chain(d):
        first = mine == (0 if d == FWD else 1)
        prev, nxt = (has[0], has[1]) if d == FWD else (has[1], has[0])

        def body(c):
            send1(d, c).wait_recv()

            @pl.when(prev)
            def _():
                sendc(d, c).wait_recv()

            @pl.when(jnp.logical_not(prev))
            def _():
                rxc[d, c] = jnp.zeros((rxc.shape[2], cw), BF16)

            dec_me = decay_row[:, my_cols(c)]
            dec_peer = decay_peer[:, my_cols(c)]
            fresh = own_ref[c]
            fresh_peer = rx1[d, c].astype(F32)
            before = rxc[d, c].astype(F32)
            after_me = dec_me * before + fresh
            after_peer = dec_peer * before + fresh_peer

            @pl.when(nxt)
            def _():
                txc[d, c] = jnp.where(
                    first, dec_peer * after_me + fresh_peer, dec_me * after_peer + fresh
                ).astype(BF16)
                sendc(d, c).start()

            tx3[d, c] = jnp.where(first, after_me, before).astype(BF16)

            @pl.when(prev)
            def _():
                send3(d, c).start()

            state_ref[d, mine * chunks + c] = jnp.where(first, before, after_peer).astype(BF16)

        for c in range(chunks):
            body(c)

    def head_sends(d):
        for c in range(chunks):
            send3(d, c).start()

    load_x.wait()
    pl.semaphore_wait(barrier, len(greet))
    dec.start()
    loads[2].wait()
    do_copies = []
    for k, peer in enumerate(chan_peers):
        do_copies.append(remote(dfull.at[0], dfull.at[k + 1], do_send.at[k], do_recv.at[k], peer))
        do_copies[-1].start()
    b_t = b_ref[...].T
    make(FWD, b_t, lambda cols: (tdt_e[:, cols] * x_ref[:, cols].astype(F32)).astype(BF16))

    scores = jnp.where(causal & (count_col == count_row), dot_cols(c_ref[...], b_ref[...]), 0.0)
    pos_lane = lax.broadcasted_iota(jnp.int32, (rows, 2 * hd), 1) < hd
    carry_e[...] = expand(carry, 2)
    loads[0].wait()

    def block_diag(pair):
        pair = pair.astype(F32)
        return jnp.concatenate(
            [jnp.where(pos_lane, pair, 0.0), jnp.where(pos_lane, 0.0, pair)], axis=0
        ).astype(BF16)

    for q in range(heads // 2):
        cols = slice(q * 2 * hd, (q + 1) * 2 * hd)
        mixes = []
        for h in (2 * q, 2 * q + 1):
            gap = jnp.minimum(running_ref[:, h : h + 1] - run_row[h : h + 1, :], 0.0)
            mixes.append((jnp.exp(gap) * scores * dt_ref[h : h + 1, :]).astype(BF16))
            mix_ref[q, (h % 2) * rows : (h % 2 + 1) * rows, :] = mixes[-1]
        pair = x_ref[:, cols]
        inside_ref[:, cols] = dot(jnp.concatenate(mixes, axis=1), block_diag(pair)) + skip_e[
            :, cols
        ] * pair.astype(F32)
        zf = z_ref[:, cols].astype(F32)
        act_ref[:, cols] = zf / (1.0 + jnp.exp(-zf))

    tile = min(256, width)

    def pull():
        loads[1].wait()
        for copy in do_copies:
            copy.wait_recv()

        def body(i, _):
            feats = pl.ds(pl.multiple_of(i * tile, tile), tile)
            total = None
            for k in range(n_chan):
                source = lax.rem(chan + n_chan - k, n_chan)
                piece = dot_cols(dfull[k], w_ref[feats, pl.ds(pl.multiple_of(source * nb, nb), nb)])
                total = piece if total is None else total + piece
            pulled_ref[:, feats] = total
            return 0

        lax.fori_loop(0, width // tile, body, 0)

    pl.when(place == last)(pull)
    dec.wait_recv()
    chain(FWD)
    pl.when(place == 0)(lambda: head_sends(FWD))
    pl.when(place < last)(pull)

    def gate(q, sums):
        squares, dots = sums
        cols = pl.ds(pl.multiple_of(q * gw, gw), gw)
        carried = jnp.concatenate(
            [dot(c_ref[...], state_ref[FWD, q * group + k]) for k in range(group)], axis=1
        )
        gated = (inside_ref[:, cols] + carry_e[:, cols] * carried) * act_ref[:, cols]
        normed = (gated * gain_ref[:, cols]).astype(BF16)
        gated_ref[:, cols] = gated
        normed_ref[:, cols] = normed
        sq = gated * gated
        od = normed.astype(F32) * pulled_ref[:, cols]
        for k in range(gw // 128):
            squares = squares + sq[:, k * 128 : (k + 1) * 128]
            dots = dots + od[:, k * 128 : (k + 1) * 128]
        return squares, dots

    zero = jnp.zeros((rows, 128), F32)
    sums = lax.fori_loop(0, groups, lambda g, s: gate(mine * groups + g, s), (zero, zero))

    def gate_late(d):
        def body(g, s):
            for k in range(group):
                send3(d, g * group + k).wait_recv()
            return gate((1 - mine) * groups + g, s)

        return body

    squares, dots = lax.fori_loop(0, groups, gate_late(FWD), sums)
    sq_col = jnp.sum(squares, axis=1, keepdims=True)
    dot_col = jnp.sum(dots, axis=1, keepdims=True)
    lane = lax.broadcasted_iota(jnp.int32, (rows, 128), 1)
    stats = jnp.where(lane == 0, sq_col, jnp.where(lane == 1, dot_col, 0.0))
    stat_tx[...] = stats.T[0:8, :]
    st_copies = []
    for k, peer in enumerate(chan_peers):
        st_copies.append(remote(stat_tx, stat_rx.at[k], st_send.at[k], st_recv.at[k], peer))
        st_copies[-1].start()
    total = stat_tx[...]
    for k, copy in enumerate(st_copies):
        copy.wait_recv()
        total = total + stat_rx[k]
    stat_cols = jnp.concatenate([total, jnp.zeros((rows - 8, rows), F32)], axis=0).T
    inv = lax.rsqrt(stat_cols[:, 0:1] / total_width + NORM_EPS)
    back = inv * inv * inv * stat_cols[:, 1:2] / total_width

    c_t = c_ref[...].T

    def cot_block(cols):
        gated = gated_ref[:, cols]
        d_normed = inv * pulled_ref[:, cols]
        d = ((gain_ref[:, cols] * d_normed - back * gated) * act_ref[:, cols]).astype(BF16)
        d_ref[:, cols] = d
        pulled_ref[:, cols] = gated * d_normed
        return (carry_e[:, cols] * d.astype(F32)).astype(BF16)

    make(BWD, c_t, cot_block)

    def cot(q, _):
        cols = pl.ds(pl.multiple_of(q * gw, gw), gw)
        red_tx[0, 0:1, cols] = jnp.sum(pulled_ref[:, cols], axis=0, keepdims=True)
        red_tx[0, 1:2, cols] = jnp.sum(
            d_ref[:, cols].astype(F32) * x_ref[:, cols].astype(F32), axis=0, keepdims=True
        )
        return 0

    lax.fori_loop(0, 2 * groups, cot, 0)

    def red(k):
        return remote(red_tx.at[k], red_rx.at[k], rd_send.at[k], rd_recv.at[k], steps[k])

    def reduce_step(k):
        red(k).wait_recv()
        red_tx[k + 1] = red_tx[k] + red_rx[k]
        if k + 1 < len(steps):
            red(k + 1).start()

    def red_far(k):
        slot = len(steps) + k
        return remote(red_tx.at[len(steps)], red_rx.at[slot], rd_send.at[slot], rd_recv.at[slot], far[k])

    red(0).start()
    tile_n = min(256, nb)

    def project(block, store):
        def body(i, _):
            at = pl.ds(pl.multiple_of(block * nb + i * tile_n, tile_n), tile_n)
            store(pl.ds(pl.multiple_of(i * tile_n, tile_n), tile_n), dot(normed_ref[...], w_ref[:, at]))
            return 0

        lax.fori_loop(0, nb // tile_n, body, 0)

    pj_copies = []
    for k, peer in enumerate(chan_peers):

        def store(at, value, k=k):
            proj_tx[k, :, at] = value.astype(BF16)

        project(peer["chan"], store)
        pj_copies.append(remote(proj_tx.at[k], proj_rx.at[k], pj_send.at[k], pj_recv.at[k], peer))
        pj_copies[-1].start()

    pl.when(place == last)(lambda: chain(BWD))
    reduce_step(0)
    def own_body(i, _):
        at = pl.ds(pl.multiple_of(chan * nb + i * tile_n, tile_n), tile_n)
        proj_own[:, pl.ds(pl.multiple_of(i * tile_n, tile_n), tile_n)] = dot(normed_ref[...], w_ref[:, at])
        return 0

    lax.fori_loop(0, nb // tile_n, own_body, 0)
    for q in range(heads // 2):
        cols = slice(q * 2 * hd, (q + 1) * 2 * hd)
        pair = d_ref[:, cols]
        inside_ref[:, cols] = dot_rows(mix_ref[q], block_diag(pair)) + skip_e[:, cols] * pair.astype(F32)

    def finish_out():
        for copy in pj_copies:
            copy.wait_recv()
        for i in range(nb // tile_n):
            at = slice(i * tile_n, (i + 1) * tile_n)
            value = proj_own[:, at]
            for k in range(n_chan - 1):
                value = value + proj_rx[k, :, at].astype(F32)
            out_ref[:, at] = (inv * value).astype(BF16)

    def settle():
        for k in range(1, len(steps)):
            reduce_step(k)
        for k in range(len(far)):
            red_far(k).start()
        finish_out()

    pl.when(place < last - 1)(settle)
    pl.when(place < last)(lambda: chain(BWD))
    pl.when(place >= last - 1)(settle)
    pl.when(place == last)(lambda: head_sends(BWD))

    def finish(q):
        cols = pl.ds(pl.multiple_of(q * gw, gw), gw)
        carried = jnp.concatenate(
            [dot(b_ref[...], state_ref[BWD, q * group + k]) for k in range(group)], axis=1
        )
        gx_ref[:, cols] = (inside_ref[:, cols] + tdt_e[:, cols] * carried).astype(BF16)

    def early(g, _):
        finish(mine * groups + g)
        return 0

    def late(g, _):
        for k in range(group):
            send3(BWD, g * group + k).wait_recv()
        finish((1 - mine) * groups + g)
        return 0

    lax.fori_loop(0, groups, early, 0)
    lax.fori_loop(0, groups, late, 0)

    final = red_tx[len(steps)]
    for k in range(len(far)):
        red_far(k).wait_recv()
        final = final + red_rx[len(steps) + k]
    gg_ref[...] = final[0:1, :]
    skip_cols = jnp.concatenate([final[1:2, :], jnp.zeros((7, width), F32)], axis=0)
    skip_sum = jnp.zeros((8, heads), F32)
    for part in split(skip_cols, 3):
        skip_sum = skip_sum + dot_cols(part, spread)
    gs_ref[...] = skip_sum[0:1, :]

    dec.wait_send()
    for copy in do_copies + st_copies + pj_copies:
        copy.wait_send()
    for k in range(len(steps)):
        red(k).wait_send()
    for k in range(len(far)):
        red_far(k).wait_send()
    for d in (FWD, BWD):
        for c in range(chunks):
            send1(d, c).wait_send()
            send3(d, c).wait_send()

            @pl.when(has[1] if d == FWD else has[0])
            def _():
                sendc(d, c).wait_send()


def hand_over(*refs):
    for source, target in zip(refs[:4], refs[4:]):
        target[...] = source[...]


def local(
    mesh_shape, ssm_input, gate_z, b_proj, c_proj, step_size, log_decay, skip_d, norm_gain, w_out, d_out, game_lengths
):
    n_seq, n_chan, n_dp = (mesh_shape[a] for a in ("seq", "chan", "dp"))
    _, rows, width = ssm_input.shape
    heads = step_size.shape[2]
    states = b_proj.shape[2]
    model = w_out.shape[1]
    nb = d_out.shape[2]
    half = width // 2
    chunks = max(1, min(8, half // 128))
    cw = half // chunks
    reds = n_dp.bit_length()
    slots = reds + n_seq // 2 - 1
    peers = max(1, n_chan - 1)
    sizes = (n_seq, n_chan, n_dp, heads, game_lengths.shape[1], chunks)
    vmem = pl.BlockSpec(memory_space=pltpu.VMEM)
    hbm = pl.BlockSpec(memory_space=pltpu.HBM)
    dma = pltpu.SemaphoreType.DMA
    out, gx, gg, gs = pl.pallas_call(
        functools.partial(kernel, sizes),
        out_shape=(
            pltpu.VMEM((rows, nb), BF16),
            pltpu.VMEM((rows, width), BF16),
            pltpu.VMEM((1, width), F32),
            pltpu.VMEM((1, heads), F32),
        ),
        in_specs=[hbm] + [vmem] * 6 + [pl.BlockSpec(memory_space=pltpu.SMEM)] + [hbm] * 3,
        out_specs=(vmem,) * 4,
        scratch_shapes=[
            pltpu.VMEM((rows, width), BF16),
            pltpu.VMEM((rows, width), BF16),
            pltpu.VMEM((width, model), BF16),
            pltpu.VMEM((n_chan, rows, nb), BF16),
            pltpu.VMEM((rows, heads), F32),
            pltpu.VMEM((heads, rows), F32),
            pltpu.VMEM((1, width), F32),
            pltpu.VMEM((1, width), F32),
            pltpu.VMEM((rows, width), F32),
            pltpu.VMEM((rows, width), F32),
            pltpu.VMEM((heads // 2, 2 * rows, rows), BF16),
            pltpu.VMEM((rows, width), F32),
            pltpu.VMEM((rows, width), F32),
            pltpu.VMEM((rows, width), F32),
            pltpu.VMEM((rows, width), BF16),
            pltpu.VMEM((rows, width), F32),
            pltpu.VMEM((rows, width), BF16),
            pltpu.VMEM((chunks, states, cw), F32),
            pltpu.VMEM((2, chunks, states, cw), BF16),
            pltpu.VMEM((2, chunks, states, cw), BF16),
            pltpu.VMEM((2, chunks, states, cw), BF16),
            pltpu.VMEM((2, chunks, states, cw), BF16),
            pltpu.VMEM((2, chunks, states, cw), BF16),
            pltpu.VMEM((2, 2 * chunks, states, cw), BF16),
            pltpu.VMEM((8, rows), F32),
            pltpu.VMEM((peers, 8, rows), F32),
            pltpu.VMEM((peers, rows, nb), BF16),
            pltpu.VMEM((peers, rows, nb), BF16),
            pltpu.VMEM((rows, nb), F32),
            pltpu.VMEM((reds + 1, 2, width), F32),
            pltpu.VMEM((slots, 2, width), F32),
            dma((3,)),
            dma,
            dma((peers,)),
            dma((peers,)),
            dma((2,)),
            dma((2, chunks)),
            dma((2, chunks)),
            dma((2, chunks)),
            dma((2, chunks)),
            dma((2, chunks)),
            dma((2, chunks)),
            dma((peers,)),
            dma((peers,)),
            dma((peers,)),
            dma((peers,)),
            dma((slots,)),
            dma((slots,)),
        ],
        compiler_params=pltpu.CompilerParams(
            collective_id=0, has_side_effects=True, vmem_limit_bytes=60 * 1024 * 1024
        ),
    )(
        ssm_input[0],
        b_proj[0],
        c_proj[0],
        step_size[0].T,
        log_decay[0].T,
        skip_d[None],
        norm_gain[None],
        game_lengths,
        gate_z[0],
        w_out,
        d_out[0],
    )
    results = (out, gx, gg, gs)
    out, gx, gg, gs = pl.pallas_call(
        hand_over,
        out_shape=tuple(jax.ShapeDtypeStruct(a.shape, a.dtype) for a in results),
        in_specs=[vmem] * 4,
        out_specs=(vmem,) * 4,
        compiler_params=pltpu.CompilerParams(vmem_limit_bytes=4 * 1024 * 1024),
    )(*results)
    return out[None], gx[None], gg[0], gs[0]


def solution(mesh):
    return jax.shard_map(
        functools.partial(local, dict(mesh.shape)),
        mesh=mesh,
        in_specs=(
            P("dp", "seq", "chan"),
            P("dp", "seq", "chan"),
            P("dp", "seq", None),
            P("dp", "seq", None),
            P("dp", "seq", "chan"),
            P("dp", "seq", "chan"),
            P("chan"),
            P("chan"),
            P("chan", None),
            P("dp", "seq", "chan"),
            P("dp", None),
        ),
        out_specs=(P("dp", "seq", "chan"), P("dp", "seq", "chan"), P("chan"), P("chan")),
        check_vma=False,
    )
```
